256 devices in a mesh: ctx: 16 (over z_hi, x), tp: 4 (over y), dp: 4 (over z_lo, core).
Axes of the slice: x: 4, y: 4, z: 8 (z_hi: 4, z_lo: 2; z = z_hi * 2 + z_lo), core: 2. Of those that a mesh axis runs over, the one named last changes fastest.
Arguments:
- byte_embed: bfloat16 [65536, 1024], P(('dp', 'ctx', 'tp')), parts along dimension 0, may hold values from -6 to 6
- patch_start: int32 [65536], P(('dp', 'ctx', 'tp')), parts along dimension 0, may hold values from 0 to 1, as said below
- enc_gain: float32 [1024], replicated, may hold values from 0.1 to 1.9
- enc_qkv: bfloat16 [1024, 3072], replicated, may hold values from -4 to 4
- enc_out: bfloat16 [1024, 1024], replicated, may hold values from -0.1875 to 0.1875
- up_proj: bfloat16 [1024, 4096], P('ctx', 'tp'), may hold values from -0.1875 to 0.1875
- lat_gain: float32 [4096], replicated, may hold values from 0.1 to 1.9
- query_proj: bfloat16 [4096, 2048], P('ctx', 'tp'), may hold values from -4 to 4
- key_proj: bfloat16 [4096, 512], P('ctx', 'tp'), may hold values from -4 to 4
- value_matrix: bfloat16 [4096, 512], P('ctx', 'tp'), may hold values from -0.09375 to 0.09375
- out_proj: bfloat16 [2048, 4096], P('tp', 'ctx'), may hold values from -0.125 to 0.125
- down_proj: bfloat16 [4096, 1024], P('tp', 'ctx'), may hold values from -0.09375 to 0.09375
Outputs:
- byte_states: bfloat16 [65536, 1024], P(('dp', 'ctx', 'tp')), parts along dimension 0
The draws below stay inside these ranges and needn't reach their ends.
There are 4 independent parts, one for each index of `dp`. The reference program is written for one: setup_inputs(seed, part) draws one part's arguments, and reference() takes and returns one part's arrays. A program takes and returns all parts, laid end to end along the dimension named above; an argument that names none is the same for every part. Nothing has to cross between parts.
Inputs may be any that keep to these rules, and one draw needn't show every extreme that they name: `patch_start`: byte 0 begins a patch; every patch spans 1 to 19 bytes; each aligned group of 1024 bytes holds at most 256 patch starts, and some group holds exactly 256.
All inputs are finite; a program needn't handle non-finite values.
Results may differ from the reference program's by a relative error of at most 0.015.
Values may be sent and summed in bfloat16 or wider, within the bound.
A program may use at most 128 MiB of HBM per device.

```python
import math
import jax
import jax.numpy as jnp
from jax import lax

DB = 1024
BH = 16
HB = 64
LATENT_WIDTH = 4096
QUERY_HEADS = 16
KEYVALUE_HEADS = 4
HEAD_SIZE = 128
WIN = 512
BYTE_DEV = 256
GROUP = 1024
CAP = 256
BYTES = 16384
SLOTS = 4096
N_CTX = 16


def draw_patch_start(key, part):
    key_prob, key_full, key_roll, key_place = jax.random.split(jax.random.fold_in(key, 7), 4)
    quads = BYTES // 4
    quad_index = jnp.arange(quads, dtype=jnp.int32)
    quad_group = quad_index // CAP
    chance = jax.random.randint(key_prob, (N_CTX,), 600, 1001)
    full_group = jax.random.randint(key_full, (), 0, N_CTX)
    chance = jnp.where(jnp.arange(N_CTX, dtype=jnp.int32) == full_group, 1000, chance)
    roll = jax.random.randint(key_roll, (quads,), 0, 1000)
    present = (roll < chance[quad_group]) | (quad_index % 4 == 0)
    place = jax.random.randint(key_place, (quads,), 0, 4)
    place = jnp.where(quad_index == 0, 0, place)
    marks = (jnp.arange(4, dtype=jnp.int32)[None, :] == place[:, None]) & present[:, None]
    return marks.reshape(BYTES).astype(jnp.int32)


def draw_byte_embed(key, part):
    key_drawn = jax.random.fold_in(jax.random.fold_in(key, 11), 0)
    simple_sample = jax.random.normal(key_drawn, (BYTES, DB), jnp.float32)
    return jnp.clip(simple_sample, -6.0, 6.0).astype(jnp.bfloat16)


def draw_enc_qkv(key, part):
    key_drawn = jax.random.fold_in(jax.random.fold_in(key, 13), 0)
    simple_sample = jax.random.normal(key_drawn, (DB, 3 * DB), jnp.float32) / math.sqrt(DB)
    return jnp.clip(simple_sample, -4.0, 4.0).astype(jnp.bfloat16)


def draw_query_proj(key, part):
    simple_sample = jax.random.normal(jax.random.fold_in(key, 31), (LATENT_WIDTH, QUERY_HEADS * HEAD_SIZE), jnp.float32) / math.sqrt(LATENT_WIDTH)
    return jnp.clip(simple_sample, -4.0, 4.0).astype(jnp.bfloat16)


def draw_key_proj(key, part):
    simple_sample = jax.random.normal(jax.random.fold_in(key, 37), (LATENT_WIDTH, KEYVALUE_HEADS * HEAD_SIZE), jnp.float32) / math.sqrt(LATENT_WIDTH)
    return jnp.clip(simple_sample, -4.0, 4.0).astype(jnp.bfloat16)


def steps_of(stream_key, dims, cuts, smallest, high):
    loudness = 1.0
    for axis_at, blocks in cuts:
        draws = jax.random.uniform(jax.random.fold_in(jax.random.fold_in(stream_key, 6), axis_at), (blocks,), jnp.float32, smallest / len(cuts), high / len(cuts))
        loudness = loudness * jnp.repeat(jnp.exp(draws), dims[axis_at] // blocks).reshape((-1,) + (1,) * (len(dims) - 1 - axis_at))
    return loudness


def noise(own_key, shape, deviation, most, pieces=(), kind=jnp.bfloat16):
    entries = jax.random.normal(own_key, shape, jnp.float32) * deviation
    if len(pieces) > 0:
        entries = steps_of(own_key, shape, pieces, -0.22, 0.18) * entries
    return jnp.clip(entries, min=-most, max=most).astype(kind)


def setup_inputs(seed: int = 0, part: int = 0) -> dict:
    seeds = jax.random.split(jax.random.key(seed), 13)
    part_splits = jax.random.split(jax.random.fold_in(seeds[12], part), 13)
    return {
        "byte_embed": draw_byte_embed(jax.random.fold_in(jax.random.fold_in(seeds[12], part), 71), part),
        "patch_start": draw_patch_start(jax.random.fold_in(jax.random.fold_in(seeds[12], part), 71), part),
        "enc_gain": jnp.clip(1.0 + 0.18 * jax.random.normal(seeds[2], (DB,), jnp.float32), 0.1, 1.9),
        "enc_qkv": draw_enc_qkv(jax.random.fold_in(seeds[12], 71), part),
        "enc_out": noise(seeds[4], (DB, DB), DB ** -0.5, 0.1875),
        "up_proj": noise(seeds[5], (DB, LATENT_WIDTH), DB ** -0.5, 0.1875, ((0, 16), (1, 4))),
        "lat_gain": jnp.clip(1.0 + 0.18 * jax.random.normal(seeds[6], (LATENT_WIDTH,), jnp.float32), 0.1, 1.9),
        "query_proj": draw_query_proj(jax.random.fold_in(seeds[12], 71), part),
        "key_proj": draw_key_proj(jax.random.fold_in(seeds[12], 71), part),
        "value_matrix": noise(seeds[9], (LATENT_WIDTH, KEYVALUE_HEADS * HEAD_SIZE), LATENT_WIDTH ** -0.5, 0.09375, ((0, 16), (1, 4))),
        "out_proj": noise(seeds[10], (QUERY_HEADS * HEAD_SIZE, LATENT_WIDTH), (QUERY_HEADS * HEAD_SIZE) ** -0.5, 0.125, ((0, 4), (1, 16))),
        "down_proj": noise(seeds[11], (LATENT_WIDTH, DB), LATENT_WIDTH ** -0.5, 0.09375, ((0, 4), (1, 16))),
    }


EPS = 1e-05

def rms_scale(values, gain):
    floats = values.astype(jnp.float32)
    return floats * lax.rsqrt(lax.optimization_barrier(jnp.mean(floats * floats, axis=-1, keepdims=True)) + EPS) * gain

def window_attend(query, keys, values, first):
    n_query = query.shape[0]
    n_key = keys.shape[0]
    qh = query.reshape(n_query, BH, HB).astype(jnp.float32)
    kh = keys.reshape(n_key, BH, HB).astype(jnp.float32)
    vh = values.reshape(n_key, BH, HB).astype(jnp.float32)
    scores = jnp.einsum('qhd,khd->hqk', qh, kh) / jnp.sqrt(jnp.float32(HB))
    q_pos = first + jnp.arange(n_query, dtype=jnp.int32)
    k_pos = first - (n_key - n_query) + jnp.arange(n_key, dtype=jnp.int32)
    allowed = (k_pos[None, :] <= q_pos[:, None]) & (k_pos[None, :] > q_pos[:, None] - WIN) & (k_pos[None, :] >= 0)
    scores = jnp.where(allowed[None], scores, jnp.float32(-1e+30))
    peak = lax.optimization_barrier(jnp.max(scores, axis=-1, keepdims=True))
    expo = jnp.where(allowed[None], jnp.exp(scores - peak), jnp.float32(0.0))
    total = lax.optimization_barrier(jnp.sum(expo, axis=-1, keepdims=True))
    weights = expo.astype(jnp.bfloat16).astype(jnp.float32)
    mixed = jnp.einsum('hqk,khd->hqd', weights, vh) / total
    return jnp.transpose(mixed, (1, 0, 2)).reshape(n_query, BH * HB).astype(jnp.bfloat16)

def reference(byte_embed, patch_start, enc_gain, enc_qkv, enc_out, up_proj, lat_gain, query_proj, key_proj, value_matrix, out_proj, down_proj):
    normed = rms_scale(byte_embed, enc_gain).astype(jnp.bfloat16)
    qkv = jnp.dot(normed, enc_qkv, preferred_element_type=jnp.float32).astype(jnp.bfloat16)
    query = qkv[:, :DB]
    keys = qkv[:, DB:2 * DB]
    values = qkv[:, 2 * DB:]
    padding = jnp.zeros((2 * BYTE_DEV, DB), jnp.bfloat16)
    key_pad = jnp.concatenate([padding, keys], axis=0)
    value_pad = jnp.concatenate([padding, values], axis=0)

    def one_block(index):
        begin = index * BYTE_DEV
        q_block = lax.dynamic_slice_in_dim(query, begin, BYTE_DEV, 0)
        k_block = lax.dynamic_slice_in_dim(key_pad, begin, 3 * BYTE_DEV, 0)
        v_block = lax.dynamic_slice_in_dim(value_pad, begin, 3 * BYTE_DEV, 0)
        return window_attend(q_block, k_block, v_block, begin)
    blocks = jnp.arange(BYTES // BYTE_DEV, dtype=jnp.int32)
    context = lax.map(one_block, blocks).reshape(BYTES, DB)
    hidden = (byte_embed.astype(jnp.float32) + jnp.dot(context, enc_out, preferred_element_type=jnp.float32)).astype(jnp.bfloat16)
    position = jnp.arange(BYTES, dtype=jnp.int32)
    group = position // GROUP
    running = jnp.cumsum(patch_start).astype(jnp.int32)
    before = running - patch_start
    base = before[jnp.arange(N_CTX, dtype=jnp.int32) * GROUP]
    slot = before - base[group]
    begin_row = jnp.where(patch_start == 1, group * CAP + slot, -1).astype(jnp.int32)
    row = lax.cummax(begin_row, axis=0)
    sums = jax.ops.segment_sum(hidden.astype(jnp.float32), row, num_segments=SLOTS)
    counts = jax.ops.segment_sum(jnp.ones((BYTES,), jnp.float32), row, num_segments=SLOTS)
    pooled = (sums / jnp.maximum(counts, 1.0)[:, None]).astype(jnp.bfloat16)
    latent = jnp.dot(pooled, up_proj, preferred_element_type=jnp.float32).astype(jnp.bfloat16)
    lnorm = rms_scale(latent, lat_gain).astype(jnp.bfloat16)
    q_all = jnp.dot(lnorm, query_proj, preferred_element_type=jnp.float32).astype(jnp.bfloat16)
    k_all = jnp.dot(lnorm, key_proj, preferred_element_type=jnp.float32).astype(jnp.bfloat16)
    v_all = jnp.dot(lnorm, value_matrix, preferred_element_type=jnp.float32).astype(jnp.bfloat16)
    used = counts > 0.0
    rows = jnp.arange(SLOTS, dtype=jnp.int32)
    allowed = used[None, :] & (rows[None, :] <= rows[:, None])

    def one_head(head_number):
        keyvalue_head = head_number // (QUERY_HEADS // KEYVALUE_HEADS)
        q_head = lax.dynamic_slice_in_dim(q_all, head_number * HEAD_SIZE, HEAD_SIZE, 1).astype(jnp.float32)
        k_head = lax.dynamic_slice_in_dim(k_all, keyvalue_head * HEAD_SIZE, HEAD_SIZE, 1).astype(jnp.float32)
        v_head = lax.dynamic_slice_in_dim(v_all, keyvalue_head * HEAD_SIZE, HEAD_SIZE, 1).astype(jnp.float32)
        scores = jnp.dot(q_head, k_head.T, precision=lax.Precision.HIGHEST) / jnp.sqrt(jnp.float32(HEAD_SIZE))
        scores = jnp.where(allowed, scores, jnp.float32(-1e+30))
        peak = lax.optimization_barrier(jnp.max(scores, axis=-1, keepdims=True))
        expo = jnp.where(allowed, jnp.exp(scores - peak), jnp.float32(0.0))
        total = lax.optimization_barrier(jnp.sum(expo, axis=-1, keepdims=True))
        weights = expo.astype(jnp.bfloat16).astype(jnp.float32)
        return (jnp.dot(weights, v_head, precision=lax.Precision.HIGHEST) / total).astype(jnp.bfloat16)
    heads = lax.map(one_head, jnp.arange(QUERY_HEADS, dtype=jnp.int32))
    attn = jnp.transpose(heads, (1, 0, 2)).reshape(SLOTS, QUERY_HEADS * HEAD_SIZE)
    latent_out = (latent.astype(jnp.float32) + jnp.dot(attn, out_proj, preferred_element_type=jnp.float32)).astype(jnp.bfloat16)
    patch_out = jnp.dot(latent_out, down_proj, preferred_element_type=jnp.float32).astype(jnp.bfloat16)
    return (hidden.astype(jnp.float32) + patch_out[row].astype(jnp.float32)).astype(jnp.bfloat16)
```

```python
import heapq

import jax
import jax.numpy as jnp
from jax import lax
from jax.experimental import pallas as pl
from jax.experimental.pallas import tpu as pltpu
from jax.sharding import PartitionSpec as P

BH = 16
HB = 64
HEAD_SIZE = 128
WIN = 512
EPS = 1e-05
MESH = pl.DeviceIdType.MESH
BF = jnp.bfloat16
F32 = jnp.float32
ROWS = 1792
HALF = ROWS // 2
A_ROWS = 448


def gather_plan(rate=46.6e3, latency=2.0):
    sizes = {"A": A_ROWS, "B": HALF - A_ROWS}
    free = {link: 0.0 for link in ("E", "I", "X+", "X-", "D")}
    heap, order, sends, halves = [], [], [], {}

    def send(now, kind, dz, dx, half, link, batch):
        rows = sizes[kind] // (1 if half is None else 2)
        end = max(now, free[link]) + rows * 512 / (650e3 if link == "D" else rate)
        free[link] = end
        sends.append((kind, dz, dx, half, link))
        batch.append(len(sends) - 1)
        heapq.heappush(heap, (end + (1.0 if link == "D" else latency), len(sends) - 1))

    def have(now, kind, dz, dx, batch):
        if kind == "A" and dx == 0:
            if dz == 0:
                send(now, "A", 0, 0, None, "E", batch)
            elif dz == 1:
                send(now, "A", 1, 0, None, "I", batch)
            elif dz == -1:
                send(now, "A", -1, 0, "other", "E", batch)
            send(now, "A", dz, 0, None, "X+", batch)
            send(now, "A", dz, 0, None, "X-", batch)
        elif kind == "A" and dx == -1:
            send(now, "A", dz, -1, 0, "X+", batch)
        elif kind == "A" and dx == 1:
            send(now, "A", dz, 1, 1, "X-", batch)
        elif kind == "B" and dz == 0:
            if dx == 0:
                send(now, "B", 0, 0, None, "X+", batch)
                send(now, "B", 0, 0, None, "X-", batch)
            elif dx == -1:
                send(now, "B", 0, -1, 0, "X+", batch)
            elif dx == 1:
                send(now, "B", 0, 1, 1, "X-", batch)
            send(now, "B", 0, dx, None, "E", batch)
        elif kind == "B" and dz == 1:
            send(now, "B", 1, dx, None, "I", batch)
        elif kind == "B" and dz == -1:
            send(now, "B", -1, dx, "other", "E", batch)
        if (dz, dx) != (0, 0):
            send(now, kind, dz, dx, None, "D", batch)

    first = []
    have(0.0, "A", 0, 0, first)
    have(0.0, "B", 0, 0, first)
    order.append((None, first))
    while heap:
        now, k = heapq.heappop(heap)
        kind, dz, dx, half, link = sends[k]
        batch = []
        if link != "D":
            if link == "E":
                dz = 1 if dz == 0 else 2
            elif link == "I":
                dz = {1: -1, 2: 2}[dz]
            elif link == "X+":
                dx = {0: -1, -1: 2}[dx]
            else:
                dx = {0: 1, 1: 2}[dx]
            if half is None:
                have(now, kind, dz, dx, batch)
            else:
                key = (kind, dz, dx)
                halves[key] = halves.get(key, 0) + 1
                if link == "E":
                    send(now, kind, 2, dx, "mine", "I", batch)
                if halves[key] == 2:
                    have(now, kind, dz, dx, batch)
        order.append((k, batch))
    return order, sends


ORDER, SENDS = gather_plan()


def enter(devices):
    barrier = pltpu.get_barrier_semaphore()
    for device in devices:
        pl.semaphore_signal(barrier, inc=1, device_id=device, device_id_type=MESH)
    pl.semaphore_wait(barrier, len(devices))


def position():
    return lax.axis_index("ctx"), lax.axis_index("tp"), lax.axis_index("dp")


def remote(src, dst, send, recv, device):
    return pltpu.make_async_remote_copy(
        src_ref=src, dst_ref=dst, send_sem=send, recv_sem=recv, device_id=device, device_id_type=MESH
    )


def normal(rows, gain):
    floats = rows.astype(F32)
    return (floats * lax.rsqrt(jnp.mean(floats * floats, axis=-1, keepdims=True) + EPS) * gain).astype(BF)


def nt(a, b):
    return lax.dot_general(a, b, (((1,), (1,)), ((), ())), preferred_element_type=F32)


def first_kernel(
    up, query_w, key_w, value_w, out_w, down_t, embed, count, gain, qkv_hbm, out_hbm,
    whole, hidden, counts,
    own, halo, relay, qkv, enc_out, normed, query, keyval, mixed, bias,
    own_sem, w_sem, g_send, g_recv, h_send, h_recv, r_send, r_recv, x_send, x_recv, c_send, c_recv,
):
    ctx, tp, dp = position()
    h, x, lo, core = ctx // 4, ctx % 4, dp // 2, dp % 2
    way = 2 * lo - 1
    turned = (1 - lo) * 2 + core
    link = {
        "E": (((h + way + 4) % 4) * 4 + x, tp, turned),
        "I": (ctx, tp, turned),
        "X+": (h * 4 + (x + 1) % 4, tp, dp),
        "X-": (h * 4 + (x + 3) % 4, tp, dp),
        "D": (ctx, tp, lo * 2 + 1 - core),
    }
    loads = [pltpu.make_async_copy(up.at[:, pl.ds(256 * i, 256)], own.at[pl.ds(64 * i, 64)], own_sem.at[i]) for i in range(4)]
    loads += [
        pltpu.make_async_copy(query_w.at[:, pl.ds(256 * i, 256)], own.at[pl.ds(256 + 256 * i, 256)], own_sem.at[4 + i])
        for i in range(2)
    ]
    loads.append(pltpu.make_async_copy(key_w, own.at[pl.ds(768, 256), pl.ds(0, 128)], own_sem.at[6]))
    loads.append(pltpu.make_async_copy(value_w, own.at[pl.ds(768, 256), pl.ds(128, 128)], own_sem.at[7]))
    loads.append(pltpu.make_async_copy(out_w, own.at[pl.ds(1024, 512)], own_sem.at[8]))
    loads += [
        pltpu.make_async_copy(down_t.at[:, pl.ds(256 * i, 256)], own.at[pl.ds(1536 + 64 * i, 64)], own_sem.at[9 + i])
        for i in range(4)
    ]
    for load in loads:
        load.start()
    weights = [pltpu.make_async_copy(qkv_hbm, qkv, w_sem.at[0]), pltpu.make_async_copy(out_hbm, enc_out, w_sem.at[1])]
    for load in weights:
        load.start()

    def copy(k):
        kind, dz, dx, half, where = SENDS[k]
        rows = A_ROWS if kind == "A" else HALF - A_ROWS
        base = core * HALF + (0 if kind == "A" else A_ROWS)
        if half is not None:
            rows = rows // 2
            base = base + {"mine": lo, "other": 1 - lo}.get(half, half) * rows
        part = pl.ds(pl.multiple_of(base, 16), rows)
        piece = whole.at[(h + dz * way + 8) % 4, (x + dx + 4) % 4, part]
        return remote(own.at[part] if (dz, dx) == (0, 0) else piece, piece, g_send.at[k], g_recv.at[k], link[where])

    last = (tp == 3).astype(jnp.int32)
    zero = (tp == 0).astype(jnp.int32)
    following = ((ctx + last) % 16, (tp + 1) % 4, dp)
    previous = ((ctx - zero + 16) % 16, (tp + 3) % 4, dp)
    tps = [(ctx, (tp + i) % 4, dp) for i in (1, 2, 3)]
    over = ((((h + 1) % 4) * 4), tp * 0, dp)
    under = [((((h + 3) % 4) * 4 + j), t, dp) for t in (2, 3) for j in range(4)]
    row_mates = [(h * 4 + j, tp, dp) for j in range(3)]
    origin = (h * 4 + 3, tp, dp)
    upper = tp >= 2
    sends_over = (x == 3) & upper
    relays = (x < 3) & upper
    takes_over = (x == 0) & (tp == 0)
    crossing = (x == 3) & (tp == 3)

    barrier = pltpu.get_barrier_semaphore()

    def greet(devices):
        for device in devices:
            pl.semaphore_signal(barrier, inc=1, device_id=device, device_id_type=MESH)

    greet([link[name] for name in ("E", "I", "X+", "X-", "D")] + [following, previous] + tps)

    @pl.when(sends_over)
    def _():
        greet(row_mates + [over])

    @pl.when(relays)
    def _():
        greet([origin, over])

    @pl.when(takes_over)
    def _():
        greet(under)

    more = 4 * sends_over.astype(jnp.int32) + 2 * relays.astype(jnp.int32) + 8 * takes_over.astype(jnp.int32)
    pl.semaphore_wait(barrier, 10 + more)

    one = remote(embed, halo.at[1], h_send.at[0], h_recv.at[0], following)
    two = remote(halo.at[1], halo.at[0], h_send.at[1], h_recv.at[1], following)
    to_relay = [remote(embed.at[pl.ds(64 * j, 64)], relay, r_send.at[j], r_recv, row_mates[j]) for j in range(3)]

    def over_copy(t, j):
        src = embed.at[pl.ds(192, 64)] if j == 3 else relay
        return remote(src, halo.at[t - 2, pl.ds(64 * j, 64)], x_send, x_recv.at[4 * (t - 2) + j], over)

    def each_over(action, columns):
        for t in (2, 3):
            for j in columns:

                @pl.when((tp == t) & (x == j))
                def _():
                    action(over_copy(t, j))

    @pl.when(sends_over)
    def _():
        for c in to_relay:
            c.start()

    each_over(lambda c: c.start(), (3,))

    @pl.when(jnp.logical_not(crossing))
    def _():
        one.start()

    for i, device in enumerate(tps):
        remote(count, counts.at[tp], c_send.at[i], c_recv.at[i], device).start()
    counts[pl.ds(tp, 1)] = count[...][None]

    def first_sends():
        for load in loads:
            load.wait()
        for s in ORDER[0][1]:
            copy(s).start()

    def project(block, rows, columns):
        normed[...] = normal(rows, gain[...])

        def tile(i, carry):
            at = pl.multiple_of(i * 256, 256)
            piece = jnp.dot(normed[...], qkv[:, pl.ds(1024 + at, 256)], preferred_element_type=F32).astype(BF)
            keyval[pl.ds(256 * block, 256), pl.ds(at, 256)] = piece
            return carry

        lax.fori_loop(0, 8, tile, 0)
        if columns:

            def query_tile(i, carry):
                at = pl.multiple_of(i * 256, 256)
                piece = jnp.dot(normed[...], qkv[:, pl.ds(at, 256)], preferred_element_type=F32)
                query[:, pl.ds(at, 256)] = (piece.astype(BF).astype(F32) * 0.125).astype(BF)
                return carry

            lax.fori_loop(0, 4, query_tile, 0)

    def own_part():
        r = lax.broadcasted_iota(jnp.int32, (256, 768), 0)
        c = lax.broadcasted_iota(jnp.int32, (256, 768), 1)
        floor = 512 - 256 * (ctx * 4 + tp)
        bias[...] = jnp.where((c <= r + 512) & (c > r) & (c >= floor), F32(0.0), F32(-1e30))
        weights[0].wait()
        project(2, embed[...], True)

    def relay_part():
        @pl.when(relays)
        def _():
            remote(embed.at[pl.ds(0, 64)], relay, r_send.at[0], r_recv, origin).wait_recv()

        each_over(lambda c: c.start(), (0, 1, 2))

    def near_part():
        @pl.when(jnp.logical_not(takes_over))
        def _():
            one.wait_recv()

        @pl.when(takes_over)
        def _():
            for j in range(4):
                over_copy(3, j).wait_recv()

        @pl.when(jnp.logical_not(crossing))
        def _():
            two.start()

        project(1, halo[1], False)

    def far_part():
        @pl.when(jnp.logical_not(takes_over))
        def _():
            two.wait_recv()

        @pl.when(takes_over)
        def _():
            for j in range(4):
                over_copy(2, j).wait_recv()

        project(0, halo[0], False)

    lanes = lax.broadcasted_iota(jnp.int32, (256, 128), 1)

    def attend(pair):
        at = pl.ds(128 * pair, 128)
        both = query[:, at]
        k = keyval[:, at]
        v = keyval[:, pl.ds(1024 + 128 * pair, 128)]
        outs = []
        for side in range(2):
            q = jnp.where((lanes < 64) == (side == 0), both, jnp.zeros_like(both))
            s = nt(q, k) + bias[...]
            e = jnp.exp(s - jnp.max(s, axis=-1, keepdims=True))
            total = jnp.sum(e, axis=-1, keepdims=True)
            outs.append(jnp.dot(e.astype(BF), v, preferred_element_type=F32) / total)
        mixed[:, at] = jnp.where(lanes < 64, outs[0], outs[1]).astype(BF)

    def finish():
        weights[1].wait()

        def tile(i, carry):
            at = pl.ds(pl.multiple_of(i * 256, 256), 256)
            piece = jnp.dot(mixed[...], enc_out[:, at], preferred_element_type=F32)
            hidden[:, at] = (embed[:, at].astype(F32) + piece).astype(BF)
            return carry

        lax.fori_loop(0, 4, tile, 0)

    jobs = {0: [own_part], 3: [relay_part], 14: [near_part], FAR: [far_part]}
    for pair in range(8):
        jobs.setdefault(FAR + 2 + 2 * pair, []).append(lambda pair=pair: attend(pair))
    jobs.setdefault(FAR + 18, []).append(finish)
    first_sends()
    keep = pltpu.make_async_copy(own, whole.at[h, x], w_sem.at[2])
    keep.start()
    done = []
    for step, (k, batch) in enumerate(ORDER):
        if step > 0:
            copy(k).wait_recv()
            for s in batch:
                copy(s).start()
        for job in jobs.get(step, []):
            job()
            done.append(job)
    for step in sorted(jobs):
        for job in jobs[step]:
            if job not in done:
                job()
    keep.wait()

    @pl.when(jnp.logical_not(crossing))
    def _():
        one.wait_send()
        two.wait_send()

    @pl.when(sends_over)
    def _():
        for c in to_relay:
            c.wait_send()

    each_over(lambda c: c.wait_send(), (0, 1, 2, 3))
    for i, device in enumerate(tps):
        remote(count, counts.at[tp], c_send.at[i], c_recv.at[i], device).wait()
    for k in range(len(SENDS)):
        copy(k).wait_send()


FAR = 46


def first_stage(up, query_w, key_w, value_w, out_w, down_t, embed, count, gain, qkv, enc_out):
    anywhere = pl.BlockSpec(memory_space=pl.ANY)
    vmem = pl.BlockSpec(memory_space=pltpu.VMEM)
    n = len(SENDS)
    dma = pltpu.SemaphoreType.DMA
    return pl.pallas_call(
        first_kernel,
        out_shape=(
            jax.ShapeDtypeStruct((4, 4, ROWS, 256), BF),
            jax.ShapeDtypeStruct(embed.shape, BF),
            jax.ShapeDtypeStruct((4, 8, 128), jnp.int32),
        ),
        in_specs=[anywhere] * 6 + [vmem] * 3 + [anywhere] * 2,
        out_specs=(anywhere, vmem, vmem),
        scratch_shapes=[
            pltpu.VMEM((ROWS, 256), BF),
            pltpu.VMEM((2, 256, 1024), BF),
            pltpu.VMEM((64, 1024), BF),
            pltpu.VMEM((1024, 3072), BF),
            pltpu.VMEM((1024, 1024), BF),
            pltpu.VMEM((256, 1024), BF),
            pltpu.VMEM((256, 1024), BF),
            pltpu.VMEM((768, 2048), BF),
            pltpu.VMEM((256, 1024), BF),
            pltpu.VMEM((256, 768), F32),
            dma((13,)), dma((3,)), dma((n,)), dma((n,)), dma((2,)), dma((2,)), dma((3,)), dma, dma, dma((8,)),
            dma((3,)), dma((3,)),
        ],
        compiler_params=pltpu.CompilerParams(collective_id=0, has_side_effects=True, vmem_limit_bytes=62 * 2**20),
    )(up, query_w, key_w, value_w, out_w, down_t, embed, count, gain, qkv, enc_out)


def second_kernel(
    hidden, marks_row, marks_col, counts, gain, weights_hbm,
    out,
    w, ones, parts, arrived, share, pooled, latent, scaled, acc, kv, kv_all, query, mx, tot, mix, attn,
    far, relay_r, relay_l, to_right, to_left, arr_r, arr_l, lat_out, downs, down_in, down_share, patch,
    lead, lead_in, trail, trail_in,
    w_sem, p_send, p_recv, s_send, s_recv, l_send, l_recv, f_send, f_recv, z_send, z_recv, x_send, x_recv,
    o_send, o_recv, d_send, d_recv, e_send, e_recv, lead_send, lead_recv, trail_send, trail_recv,
):
    ctx, tp, dp = position()
    h, x = ctx // 4, ctx % 4
    load = pltpu.make_async_copy(weights_hbm, w, w_sem)
    load.start()
    tps = [(ctx, (tp + i) % 4, dp) for i in (1, 2, 3)]
    up_y, down_y = tps[0], tps[2]
    zs = [(((h + i) % 4) * 4 + x, tp, dp) for i in (1, 3, 2)]
    right, left = (h * 4 + (x + 1) % 4, tp, dp), (h * 4 + (x + 3) % 4, tp, dp)
    next_first = ((ctx + 1) % 16, tp * 0, dp)
    before_all = [((ctx + 15) % 16, t, dp) for t in range(4)]
    barrier = pltpu.get_barrier_semaphore()

    def greet(devices):
        for device in devices:
            pl.semaphore_signal(barrier, inc=1, device_id=device, device_id_type=MESH)

    greet(tps + zs + [right, left, next_first])

    @pl.when(tp == 0)
    def _():
        greet(before_all)

    def dot(a, b):
        return jnp.dot(a, b, preferred_element_type=F32)

    def iota(shape, dim):
        return lax.broadcasted_iota(jnp.int32, shape, dim).astype(F32)

    ones[...] = jnp.ones_like(ones)
    r256, c256 = iota((256, 256), 0), iota((256, 256), 1)
    c4 = [counts[t].astype(F32) for t in range(4)]
    offset = jnp.zeros((8, 128), F32)
    for t in range(4):
        offset = offset + jnp.where(tp > t, c4[t], F32(0.0))
    group = c4[0] + c4[1] + c4[2] + c4[3]
    offset, group_one = offset[0:1, 0:1], group[0:1, 0:1]
    run_row = dot(marks_row[...], (r256 <= c256).astype(BF))
    run_col = dot((r256 >= c256).astype(BF), marks_col[...])[:, 0:1]
    slot_row = run_row[0:1] + offset - 1.0
    slot_col = run_col + offset - 1.0
    place = (r256 == slot_row).astype(BF)
    mass = dot(place, hidden[...])
    number = dot(place, ones[...])
    for t in range(4):
        parts[t, :, pl.ds(0, 1024)] = mass[64 * t : 64 * t + 64].astype(BF)
        parts[t, :, pl.ds(1024, 128)] = number[64 * t : 64 * t + 64].astype(BF)
    leading = (run_row == 0.0).astype(BF)
    lead[:, pl.ds(0, 1024)] = dot(leading, hidden[...])
    lead[:, pl.ds(1024, 128)] = dot(leading, ones[...])

    pl.semaphore_wait(barrier, 9 + 4 * (tp == 0).astype(jnp.int32))

    leads = [remote(lead, lead_in, lead_send.at[t], lead_recv, before_all[t]) for t in range(4)]

    @pl.when(tp == 0)
    def _():
        for c in leads:
            c.start()

    def scatter(src, dst, send, recv):
        return [remote(src.at[(tp + i + 1) % 4], dst.at[tp], send.at[i], recv.at[i], tps[i]) for i in range(3)]

    def spread(src, dst, send, recv):
        return [remote(src, dst.at[tp], send.at[i], recv.at[i], tps[i]) for i in range(3)]

    first = scatter(parts, arrived, p_send, p_recv)
    for c in first:
        c.start()
    arrived[pl.ds(tp, 1)] = parts[pl.ds(tp, 1)]
    for c in first:
        c.wait_recv()
    leads[0].wait_recv()
    sums = arrived[0].astype(F32) + arrived[1].astype(F32) + arrived[2].astype(F32) + arrived[3].astype(F32)
    my_row = iota((64, 1152), 0) + (64 * tp).astype(F32)
    sums = sums + jnp.where(my_row == group_one - 1.0, lead_in[0:1], F32(0.0))
    share[...] = (sums[:, :1024] / jnp.maximum(sums[:, 1024:1025], 1.0)).astype(BF)
    second = spread(share, pooled, s_send, s_recv)
    for c in second:
        c.start()
    pooled[pl.ds(tp, 1)] = share[...][None]
    load.wait()
    for c in second:
        c.wait_recv()

    def columns(t, i):
        return pl.ds(pl.multiple_of(1024 * t + 256 * i, 256), 256)

    def sent(i):
        block = latent.at[:, columns(tp, i)]
        return [
            remote(block, block, l_send.at[i], l_recv.at[i], up_y),
            remote(block, block, l_send.at[4 + i], l_recv.at[4 + i], down_y),
        ]

    def passed(i):
        block = latent.at[:, columns((tp + 3) % 4 if i < 2 else (tp + 1) % 4, i)]
        return remote(block, block, f_send.at[i], f_recv.at[i], up_y if i < 2 else down_y)

    all_pooled = pooled[...].reshape(256, 1024)
    for i in range(4):
        block = w[:, :, pl.ds(64 * i, 64), :].reshape(1024, 256)
        latent[:, columns(tp, i)] = dot(all_pooled, block).astype(BF)
        for c in sent(i):
            c.start()

    def contract(t, i, fresh=False):
        values = latent[:, columns(t, i)].astype(F32)
        inputs = (values * gain[:, columns(t, i)]).astype(BF)
        power = jnp.sum(values * values, axis=-1, keepdims=True)
        scaled[...] = power if fresh else scaled[...] + power
        for b in range(3):
            term = dot(inputs, w[t, i, pl.ds(256 + 256 * b, 256), :])
            acc[b] = term if fresh else acc[b] + term

    for i in range(4):
        contract(tp, i, i == 0)
    for i in range(4):
        remote(latent.at[:, columns(tp, i)], latent.at[:, columns(tp, i)], l_send.at[i], l_recv.at[i], up_y).wait_recv()
        if i < 2:
            passed(i).start()
        remote(latent.at[:, columns(tp, i)], latent.at[:, columns(tp, i)], l_send.at[4 + i], l_recv.at[4 + i], down_y).wait_recv()
        if i >= 2:
            passed(i).start()
        contract((tp + 3) % 4, i)
        contract((tp + 1) % 4, i)
    for i in (0, 2, 1, 3):
        passed(i).wait_recv()
        contract((tp + 2) % 4, i)
    scale = lax.rsqrt(scaled[...] * F32(1.0 / 4096.0) + EPS)
    kv[pl.ds(0, 256)] = (acc[2] * scale).astype(BF)
    kv[pl.ds(256, 16)] = jnp.broadcast_to(group_one, (16, 256)).astype(BF)

    z_copies = [remote(kv, kv_all.at[h, x], z_send.at[i], z_recv.at[i], zs[i]) for i in range(3)]
    for c in z_copies:
        c.start()

    def across(j, dz):
        z = (h + dz) % 4
        src = kv if dz == 0 else kv_all.at[z, x]
        lower, upper = pl.ds(0, 128), pl.ds(128, 144)
        a, b = (x + 3) % 4, (x + 1) % 4
        return [
            remote(src, kv_all.at[z, x], x_send.at[4 * j], x_recv.at[4 * j], right),
            remote(src, kv_all.at[z, x], x_send.at[4 * j + 1], x_recv.at[4 * j + 1], left),
            remote(kv_all.at[z, a, lower], kv_all.at[z, a, lower], x_send.at[4 * j + 2], x_recv.at[4 * j + 2], right),
            remote(kv_all.at[z, b, upper], kv_all.at[z, b, upper], x_send.at[4 * j + 3], x_recv.at[4 * j + 3], left),
        ]

    turns = (0, 3, 1, 2)
    sets = [across(j, dz) for j, dz in enumerate(turns)]
    sets[0][0].start()
    sets[0][1].start()
    kv_all[pl.ds(h, 1), pl.ds(x, 1)] = kv[...][None, None]
    for head in range(4):
        q = acc[head // 2][:, 128 * (head % 2) : 128 * (head % 2) + 128] * scale
        query[head] = q.astype(BF)

    shrink = F32(1.0) / jnp.sqrt(F32(HEAD_SIZE))

    def attend(dz, dx, fresh=False):
        z, xx = (h + dz) % 4, (x + dx) % 4
        other = z * 4 + xx

        @pl.when(other <= ctx)
        def _():
            keys = kv_all[z, xx, pl.ds(0, 256), pl.ds(0, 128)]
            values = kv_all[z, xx, pl.ds(0, 256), pl.ds(128, 128)]
            limit = kv_all[z, xx, pl.ds(256, 16), :][0:1].astype(F32)
            allowed = c256 < limit
            if fresh:
                allowed = allowed & (c256 <= r256)
            bias = jnp.where(allowed, F32(0.0), F32(-1e30))

            def one_head(head, carry):
                s = nt(query[head], keys) * shrink + bias
                peak = jnp.max(s, axis=-1, keepdims=True)
                if not fresh:
                    old = mx[head]
                    peak = jnp.maximum(peak, old)
                e = jnp.exp(s - peak)
                total = jnp.sum(e, axis=-1, keepdims=True)
                mixed = dot(e.astype(BF), values)
                if not fresh:
                    fade = jnp.exp(old - peak)
                    total = total + tot[head] * fade
                    mixed = mixed + mix[head] * fade
                mx[head] = peak
                tot[head] = total
                mix[head] = mixed
                return carry

            lax.fori_loop(0, 4, one_head, 0)

    attend(0, 0, True)
    for j in range(4):
        if j > 0:
            z_copies[j - 1].wait_recv()
            sets[j][0].start()
            sets[j][1].start()
            for i in (0, 1):
                sets[j - 1][i].wait_recv()
                sets[j - 1][i + 2].start()
            attend(turns[j], 0)
            attend(turns[j - 1], 3)
            attend(turns[j - 1], 1)
    for i in (0, 1):
        sets[3][i].wait_recv()
        sets[3][i + 2].start()
    attend(turns[3], 3)
    attend(turns[3], 1)
    for j in range(4):
        for i in (2, 3):
            sets[j][i].wait_recv()
        attend(turns[j], 2)
    for head in range(4):
        attn[:, pl.ds(128 * head, 128)] = (mix[head] / tot[head]).astype(BF)

    def part(t, i):
        return dot(attn[...], w[t, i, pl.ds(1024, 512), :])

    def block(i):
        return pl.ds(256 * i, 256)

    opposite, above, below = (tp + 2) % 4, (tp + 1) % 4, (tp + 3) % 4
    low, high = pl.ds(0, 128), pl.ds(128, 128)
    for i in range(4):
        far[:, block(i)] = part(opposite, i).astype(BF)
    o_copies = [
        remote(far.at[low], relay_r, o_send.at[0], o_recv.at[0], up_y),
        remote(far.at[high], relay_l, o_send.at[1], o_recv.at[1], down_y),
        remote(to_right, arr_r, o_send.at[2], o_recv.at[2], up_y),
        remote(to_left, arr_l, o_send.at[3], o_recv.at[3], down_y),
    ]
    o_copies[0].start()
    o_copies[1].start()
    for i in range(4):
        acc_r = part(above, i)
        if i == 0:
            o_copies[0].wait_recv()
        to_right[low, block(i)] = (acc_r[:128] + relay_r[:, block(i)].astype(F32)).astype(BF)
        to_right[high, block(i)] = acc_r[128:].astype(BF)
    o_copies[2].start()
    for i in range(4):
        acc_l = part(below, i)
        if i == 0:
            o_copies[1].wait_recv()
        to_left[low, block(i)] = acc_l[:128].astype(BF)
        to_left[high, block(i)] = (acc_l[128:] + relay_l[:, block(i)].astype(F32)).astype(BF)
    o_copies[3].start()
    o_copies[2].wait_recv()
    o_copies[3].wait_recv()
    total_down = jnp.zeros((256, 1024), F32)
    for i in range(4):
        value = part(tp, i) + latent[:, columns(tp, i)].astype(F32)
        value = value + arr_r[:, block(i)].astype(F32) + arr_l[:, block(i)].astype(F32)
        lat_out[:, block(i)] = value.astype(BF)
    for i in range(4):
        down = w[:, :, pl.ds(1536 + 64 * i, 64), :].reshape(1024, 256)
        total_down = total_down + nt(lat_out[:, block(i)], down)
    for t in range(4):
        downs[t] = total_down[64 * t : 64 * t + 64].astype(BF)
    third = scatter(downs, down_in, d_send, d_recv)
    for c in third:
        c.start()
    down_in[pl.ds(tp, 1)] = downs[pl.ds(tp, 1)]
    for c in third:
        c.wait_recv()
    sums = down_in[0].astype(F32) + down_in[1].astype(F32) + down_in[2].astype(F32) + down_in[3].astype(F32)
    down_share[...] = sums.astype(BF)
    fourth = spread(down_share, patch, e_send, e_recv)
    for c in fourth:
        c.start()
    patch[pl.ds(tp, 1)] = down_share[...][None]
    for c in fourth:
        c.wait_recv()
    patch_out = patch[...].reshape(256, 1024)
    final = (iota((16, 256), 1) == group_one - 1.0).astype(BF)
    trail[...] = dot(final, patch_out).astype(BF)
    trail_copy = remote(trail, trail_in, trail_send, trail_recv, next_first)

    @pl.when(tp == 3)
    def _():
        trail_copy.start()

    result = hidden[...].astype(F32) + dot((c256 == slot_col).astype(BF), patch_out)
    out[...] = result.astype(BF)

    @pl.when(tp == 0)
    def _():
        trail_copy.wait_recv()
        row = trail_in[...][0:1].astype(F32)
        out[...] = (out[...].astype(F32) + jnp.where(run_col == 0.0, row, F32(0.0))).astype(BF)

    @pl.when(tp == 3)
    def _():
        trail_copy.wait_send()

    @pl.when(tp == 0)
    def _():
        for c in leads:
            c.wait_send()

    for c in first + second + third + fourth + z_copies + o_copies:
        c.wait_send()
    for i in range(4):
        for c in sent(i):
            c.wait_send()
        passed(i).wait_send()
    for group_of in sets:
        for c in group_of:
            c.wait_send()


def second_stage(hidden, marks_row, marks_col, counts, gain, weights):
    anywhere = pl.BlockSpec(memory_space=pl.ANY)
    vmem = pl.BlockSpec(memory_space=pltpu.VMEM)
    dma = pltpu.SemaphoreType.DMA

    def v(*shape, kind=BF):
        return pltpu.VMEM(shape, kind)

    return pl.pallas_call(
        second_kernel,
        out_shape=jax.ShapeDtypeStruct(hidden.shape, BF),
        in_specs=[vmem] * 5 + [anywhere],
        out_specs=vmem,
        scratch_shapes=[
            v(4, 4, ROWS, 256), v(256, 128), v(4, 64, 1152), v(4, 64, 1152), v(64, 1024), v(4, 64, 1024),
            v(256, 4096), v(256, 1, kind=F32), v(3, 256, 256, kind=F32), v(272, 256), v(4, 4, 272, 256),
            v(4, 256, 128), v(4, 256, 1, kind=F32), v(4, 256, 1, kind=F32), v(4, 256, 128, kind=F32), v(256, 512),
            v(256, 1024), v(128, 1024), v(128, 1024), v(256, 1024), v(256, 1024), v(256, 1024), v(256, 1024),
            v(256, 1024), v(4, 64, 1024), v(4, 64, 1024), v(64, 1024), v(4, 64, 1024),
            v(16, 1152, kind=F32), v(16, 1152, kind=F32), v(16, 1024), v(16, 1024),
            dma, dma((3,)), dma((3,)), dma((3,)), dma((3,)), dma((8,)), dma((8,)), dma((4,)), dma((4,)),
            dma((3,)), dma((3,)), dma((16,)), dma((16,)), dma((4,)), dma((4,)), dma((3,)), dma((3,)),
            dma((3,)), dma((3,)), dma((4,)), dma, dma, dma,
        ],
        compiler_params=pltpu.CompilerParams(collective_id=1, has_side_effects=True, vmem_limit_bytes=62 * 2**20),
    )(hidden, marks_row, marks_col, counts, gain, weights)


def local(
    byte_embed, patch_start, enc_gain, enc_qkv, enc_out, up_proj, lat_gain, query_proj, key_proj,
    value_matrix, out_proj, down_proj,
):
    local_count = jnp.sum(patch_start)
    whole, hidden, counts = first_stage(
        up_proj, query_proj, key_proj, value_matrix, out_proj, down_proj.T, byte_embed,
        jnp.full((8, 128), local_count, jnp.int32), enc_gain[None, :], enc_qkv, enc_out,
    )
    marks = patch_start.astype(BF)
    marks_row = jnp.broadcast_to(marks[None, :], (16, 256))
    marks_col = jnp.broadcast_to(marks[:, None], (256, 128))
    return second_stage(hidden, marks_row, marks_col, counts, lat_gain[None, :], whole)


def solution(mesh):
    placed = (
        P(("dp", "ctx", "tp"), None), P(("dp", "ctx", "tp")), P(), P(), P(), P("ctx", "tp"), P(),
        P("ctx", "tp"), P("ctx", "tp"), P("ctx", "tp"), P("tp", "ctx"), P("tp", "ctx"),
    )
    return jax.shard_map(
        local, mesh=mesh, in_specs=placed, out_specs=P(("dp", "ctx", "tp"), None), check_vma=False
    )
```

```python
import heapq

import jax
import jax.numpy as jnp
from jax import lax
from jax.experimental import pallas as pl
from jax.experimental.pallas import tpu as pltpu
from jax.sharding import PartitionSpec as P

BH = 16
HB = 64
HEAD_SIZE = 128
WIN = 512
EPS = 1e-05
MESH = pl.DeviceIdType.MESH
BF = jnp.bfloat16
F32 = jnp.float32
FIRST, SECOND = 1024, 768


def gather_plan(whole_rows, rate=46.6e3, latency=2.0):
    sizes = {"A": whole_rows // 4, "B": whole_rows // 4}
    free = {link: 0.0 for link in ("E", "I", "X+", "X-", "D")}
    heap, order, sends, halves = [], [], [], {}

    def send(now, kind, dz, dx, half, link, batch):
        rows = sizes[kind] // (1 if half is None else 2)
        end = max(now, free[link]) + rows * 512 / (650e3 if link == "D" else rate)
        free[link] = end
        sends.append((kind, dz, dx, half, link))
        batch.append(len(sends) - 1)
        heapq.heappush(heap, (end + (1.0 if link == "D" else latency), len(sends) - 1))

    def have(now, kind, dz, dx, batch):
        if kind == "A" and dx == 0:
            if dz == 0:
                send(now, "A", 0, 0, None, "E", batch)
            elif dz == 1:
                send(now, "A", 1, 0, None, "I", batch)
            elif dz == -1:
                send(now, "A", -1, 0, "other", "E", batch)
            send(now, "A", dz, 0, None, "X+", batch)
            send(now, "A", dz, 0, None, "X-", batch)
        elif kind == "A" and dx == -1:
            send(now, "A", dz, -1, 0, "X+", batch)
        elif kind == "A" and dx == 1:
            send(now, "A", dz, 1, 1, "X-", batch)
        elif kind == "B" and dz == 0:
            if dx == 0:
                send(now, "B", 0, 0, None, "X+", batch)
                send(now, "B", 0, 0, None, "X-", batch)
            elif dx == -1:
                send(now, "B", 0, -1, 0, "X+", batch)
            elif dx == 1:
                send(now, "B", 0, 1, 1, "X-", batch)
            send(now, "B", 0, dx, None, "E", batch)
        elif kind == "B" and dz == 1:
            send(now, "B", 1, dx, None, "I", batch)
        elif kind == "B" and dz == -1:
            send(now, "B", -1, dx, "other", "E", batch)
        if (dz, dx) != (0, 0):
            send(now, kind, dz, dx, None, "D", batch)

    first = []
    have(0.0, "A", 0, 0, first)
    have(0.0, "B", 0, 0, first)
    order.append((0.0, None, first))
    while heap:
        now, k = heapq.heappop(heap)
        kind, dz, dx, half, link = sends[k]
        batch = []
        if link != "D":
            if link == "E":
                dz = 1 if dz == 0 else 2
            elif link == "I":
                dz = {1: -1, 2: 2}[dz]
            elif link == "X+":
                dx = {0: -1, -1: 2}[dx]
            else:
                dx = {0: 1, 1: 2}[dx]
            if half is None:
                have(now, kind, dz, dx, batch)
            else:
                key = (kind, dz, dx)
                halves[key] = halves.get(key, 0) + 1
                if link == "E":
                    send(now, kind, 2, dx, "mine", "I", batch)
                if halves[key] == 2:
                    have(now, kind, dz, dx, batch)
        order.append((now, k, batch))
    return order, sends


PLANS = {FIRST: gather_plan(FIRST), SECOND: gather_plan(SECOND, 38e3, 2.5)}


def enter(devices):
    barrier = pltpu.get_barrier_semaphore()
    for device in devices:
        pl.semaphore_signal(barrier, inc=1, device_id=device, device_id_type=MESH)
    pl.semaphore_wait(barrier, len(devices))


def position():
    return lax.axis_index("ctx"), lax.axis_index("tp"), lax.axis_index("dp")


def remote(src, dst, send, recv, device):
    return pltpu.make_async_remote_copy(
        src_ref=src, dst_ref=dst, send_sem=send, recv_sem=recv, device_id=device, device_id_type=MESH
    )


def gather_links(ctx, tp, dp):
    h, x, lo, core = ctx // 4, ctx % 4, dp // 2, dp % 2
    way = 2 * lo - 1
    turned = (1 - lo) * 2 + core
    return {
        "E": (((h + way + 4) % 4) * 4 + x, tp, turned),
        "I": (ctx, tp, turned),
        "X+": (h * 4 + (x + 1) % 4, tp, dp),
        "X-": (h * 4 + (x + 3) % 4, tp, dp),
        "D": (ctx, tp, lo * 2 + 1 - core),
    }


class Gather:
    def __init__(self, own, whole, send, recv):
        self.own, self.whole, self.send, self.recv = own, whole, send, recv
        self.order, self.sends = PLANS[own.shape[0]]
        self.at = 0

    def copy(self, k):
        ctx, tp, dp = position()
        h, x, lo, core = ctx // 4, ctx % 4, dp // 2, dp % 2
        kind, dz, dx, half, where = self.sends[k]
        rows = self.own.shape[0] // 4
        base = core * 2 * rows + (0 if kind == "A" else rows)
        if half is not None:
            rows = rows // 2
            base = base + {"mine": lo, "other": 1 - lo}.get(half, half) * rows
        part = pl.ds(pl.multiple_of(base, 16), rows)
        piece = self.whole.at[(h + dz * (2 * lo - 1) + 8) % 4, (x + dx + 4) % 4, part]
        device = gather_links(ctx, tp, dp)[where]
        src = self.own.at[part] if (dz, dx) == (0, 0) else piece
        return remote(src, piece, self.send.at[k], self.recv.at[k], device)

    def until(self, time):
        while self.at < len(self.order) and self.order[self.at][0] <= time:
            _, k, batch = self.order[self.at]
            if k is not None:
                self.copy(k).wait_recv()
            for s in batch:
                self.copy(s).start()
            self.at += 1

    def drain(self):
        for k in range(len(self.sends)):
            self.copy(k).wait_send()


def normal(rows, gain):
    floats = rows.astype(F32)
    return (floats * lax.rsqrt(jnp.mean(floats * floats, axis=-1, keepdims=True) + EPS) * gain).astype(BF)


def nt(a, b):
    return lax.dot_general(a, b, (((1,), (1,)), ((), ())), preferred_element_type=F32)


def first_kernel(
    up, query_w, key_w, value_w, embed, count, gain, qkv_hbm, out_hbm,
    whole, hidden, counts,
    own, halo, relay, qkv, enc_out, normed, query, keyval, mixed, bias, peaks_of, totals_of, sums_of,
    own_sem, w_sem, g_send, g_recv, h_send, h_recv, r_send, r_recv, x_send, x_recv, c_send, c_recv,
):
    ctx, tp, dp = position()
    h, x = ctx // 4, ctx % 4
    link = gather_links(ctx, tp, dp)
    loads = [pltpu.make_async_copy(up.at[:, pl.ds(256 * i, 256)], own.at[pl.ds(64 * i, 64)], own_sem.at[i]) for i in range(4)]
    loads += [
        pltpu.make_async_copy(query_w.at[:, pl.ds(256 * i, 256)], own.at[pl.ds(256 + 256 * i, 256)], own_sem.at[4 + i])
        for i in range(2)
    ]
    loads.append(pltpu.make_async_copy(key_w, own.at[pl.ds(768, 256), pl.ds(0, 128)], own_sem.at[6]))
    loads.append(pltpu.make_async_copy(value_w, own.at[pl.ds(768, 256), pl.ds(128, 128)], own_sem.at[7]))
    for load in loads:
        load.start()
    weights = [pltpu.make_async_copy(qkv_hbm, qkv, w_sem.at[0]), pltpu.make_async_copy(out_hbm, enc_out, w_sem.at[1])]
    for load in weights:
        load.start()

    gather = Gather(own, whole, g_send, g_recv)
    last = (tp == 3).astype(jnp.int32)
    zero = (tp == 0).astype(jnp.int32)
    following = ((ctx + last) % 16, (tp + 1) % 4, dp)
    previous = ((ctx - zero + 16) % 16, (tp + 3) % 4, dp)
    tps = [(ctx, (tp + i) % 4, dp) for i in (1, 2, 3)]
    over = ((((h + 1) % 4) * 4), tp * 0, dp)
    under = [((((h + 3) % 4) * 4 + j), t, dp) for t in (2, 3) for j in range(4)]
    row_mates = [(h * 4 + j, tp, dp) for j in range(3)]
    origin = (h * 4 + 3, tp, dp)
    upper = tp >= 2
    sends_over = (x == 3) & upper
    relays = (x < 3) & upper
    takes_over = (x == 0) & (tp == 0)
    crossing = (x == 3) & (tp == 3)

    barrier = pltpu.get_barrier_semaphore()

    def greet(devices):
        for device in devices:
            pl.semaphore_signal(barrier, inc=1, device_id=device, device_id_type=MESH)

    greet([link[name] for name in ("E", "I", "X+", "X-", "D")] + [following, previous] + tps)

    @pl.when(sends_over)
    def _():
        greet(row_mates + [over])

    @pl.when(relays)
    def _():
        greet([origin, over])

    @pl.when(takes_over)
    def _():
        greet(under)

    more = 4 * sends_over.astype(jnp.int32) + 2 * relays.astype(jnp.int32) + 8 * takes_over.astype(jnp.int32)
    pl.semaphore_wait(barrier, 10 + more)

    one = remote(embed, halo.at[1], h_send.at[0], h_recv.at[0], following)
    two = remote(halo.at[1], halo.at[0], h_send.at[1], h_recv.at[1], following)
    to_relay = [remote(embed.at[pl.ds(64 * j, 64)], relay, r_send.at[j], r_recv, row_mates[j]) for j in range(3)]

    def over_copy(t, j):
        src = embed.at[pl.ds(192, 64)] if j == 3 else relay
        return remote(src, halo.at[t - 2, pl.ds(64 * j, 64)], x_send, x_recv.at[4 * (t - 2) + j], over)

    def each_over(action, columns):
        for t in (2, 3):
            for j in columns:

                @pl.when((tp == t) & (x == j))
                def _():
                    action(over_copy(t, j))

    @pl.when(sends_over)
    def _():
        for c in to_relay:
            c.start()

    each_over(lambda c: c.start(), (3,))

    @pl.when(jnp.logical_not(crossing))
    def _():
        one.start()

    for i, device in enumerate(tps):
        remote(count, counts.at[tp], c_send.at[i], c_recv.at[i], device).start()
    counts[pl.ds(tp, 1)] = count[...][None]

    def first_sends():
        for load in loads:
            load.wait()
        gather.until(0.0)

    def project(block, rows, columns):
        normed[...] = normal(rows, gain[...])

        def tile(i, carry):
            at = pl.multiple_of(i * 256, 256)
            piece = jnp.dot(normed[...], qkv[:, pl.ds(1024 + at, 256)], preferred_element_type=F32).astype(BF)
            keyval[pl.ds(256 * block, 256), pl.ds(at, 256)] = piece
            return carry

        lax.fori_loop(0, 8, tile, 0)
        if columns:

            def query_tile(i, carry):
                at = pl.multiple_of(i * 256, 256)
                piece = jnp.dot(normed[...], qkv[:, pl.ds(at, 256)], preferred_element_type=F32)
                query[:, pl.ds(at, 256)] = (piece.astype(BF).astype(F32) * 0.125).astype(BF)
                return carry

            lax.fori_loop(0, 4, query_tile, 0)

    def own_part():
        r = lax.broadcasted_iota(jnp.int32, (256, 768), 0)
        c = lax.broadcasted_iota(jnp.int32, (256, 768), 1)
        floor = 512 - 256 * (ctx * 4 + tp)
        bias[...] = jnp.where((c <= r + 512) & (c > r) & (c >= floor), F32(0.0), F32(-1e30))
        weights[0].wait()
        project(2, embed[...], True)

    def relay_part():
        @pl.when(relays)
        def _():
            remote(embed.at[pl.ds(0, 64)], relay, r_send.at[0], r_recv, origin).wait_recv()

        each_over(lambda c: c.start(), (0, 1, 2))

    def near_part():
        @pl.when(jnp.logical_not(takes_over))
        def _():
            one.wait_recv()

        @pl.when(takes_over)
        def _():
            for j in range(4):
                over_copy(3, j).wait_recv()

        @pl.when(jnp.logical_not(crossing))
        def _():
            two.start()

        project(1, halo[1], False)

    def far_part():
        @pl.when(jnp.logical_not(takes_over))
        def _():
            two.wait_recv()

        @pl.when(takes_over)
        def _():
            for j in range(4):
                over_copy(2, j).wait_recv()

        project(0, halo[0], False)

    lanes = lax.broadcasted_iota(jnp.int32, (256, 128), 1)

    def attend(block, pair, carry):
        at = pl.ds(pl.multiple_of(128 * pair, 128), 128)
        rows = pl.ds(256 * block, 256)
        both = query[:, at]
        k = keyval[rows, at]
        v = keyval[rows, pl.ds(pl.multiple_of(1024 + 128 * pair, 128), 128)]
        peaks, totals, outs, fades = [], [], [], []
        for side in range(2):
            q = jnp.where((lanes < 64) == (side == 0), both, jnp.zeros_like(both))
            s = nt(q, k) + bias[:, rows]
            peak = jnp.max(s, axis=-1, keepdims=True)
            if block != 2:
                old = peaks_of[:, at][:, 64 * side : 64 * side + 1]
                peak = jnp.maximum(peak, old)
                fades.append(jnp.exp(old - peak))
            e = jnp.exp(s - peak)
            peaks.append(peak)
            totals.append(jnp.sum(e, axis=-1, keepdims=True))
            outs.append(jnp.dot(e.astype(BF), v, preferred_element_type=F32))
        first = lanes < 64
        total, out = jnp.where(first, *totals), jnp.where(first, *outs)
        if block != 2:
            fade = jnp.where(first, *fades)
            total = total + totals_of[:, at] * fade
            out = out + sums_of[:, at] * fade
        if block == 0:
            mixed[:, at] = (out / total).astype(BF)
        else:
            peaks_of[:, at] = jnp.where(first, *peaks)
            totals_of[:, at] = total
            sums_of[:, at] = out
        return carry

    def attend_block(block, times):
        for i, time in enumerate(times):
            n = 8 // len(times)
            lax.fori_loop(n * i, n * i + n, lambda pair, carry: attend(block, pair, carry), 0)
            gather.until(time)

    def finish():
        weights[1].wait()

        def tile(i, carry):
            at = pl.ds(pl.multiple_of(i * 256, 256), 256)
            piece = jnp.dot(mixed[...], enc_out[:, at], preferred_element_type=F32)
            hidden[:, at] = (embed[:, at].astype(F32) + piece).astype(BF)
            return carry

        lax.fori_loop(0, 4, tile, 0)

    own_part()
    relay_part()
    first_sends()
    keep = pltpu.make_async_copy(own, whole.at[h, x], w_sem.at[2])
    keep.start()
    attend_block(2, (2.0, 4.0, 6.0, 8.0))
    near_part()
    gather.until(10.0)
    attend_block(1, (13.0, 16.0, 19.0, 22.0))
    far_part()
    gather.until(26.0)
    attend_block(0, (28.0, 30.0, 33.0, 36.0))
    finish()
    gather.until(1000.0)
    keep.wait()

    @pl.when(jnp.logical_not(crossing))
    def _():
        one.wait_send()
        two.wait_send()

    @pl.when(sends_over)
    def _():
        for c in to_relay:
            c.wait_send()

    each_over(lambda c: c.wait_send(), (0, 1, 2, 3))
    for i, device in enumerate(tps):
        remote(count, counts.at[tp], c_send.at[i], c_recv.at[i], device).wait()
    gather.drain()


def first_stage(up, query_w, key_w, value_w, embed, count, gain, qkv, enc_out):
    anywhere = pl.BlockSpec(memory_space=pl.ANY)
    vmem = pl.BlockSpec(memory_space=pltpu.VMEM)
    n = len(PLANS[FIRST][1])
    dma = pltpu.SemaphoreType.DMA
    return pl.pallas_call(
        first_kernel,
        out_shape=(
            jax.ShapeDtypeStruct((4, 4, FIRST, 256), BF),
            jax.ShapeDtypeStruct(embed.shape, BF),
            jax.ShapeDtypeStruct((4, 8, 128), jnp.int32),
        ),
        in_specs=[anywhere] * 4 + [vmem] * 3 + [anywhere] * 2,
        out_specs=(anywhere, vmem, vmem),
        scratch_shapes=[
            pltpu.VMEM((FIRST, 256), BF),
            pltpu.VMEM((2, 256, 1024), BF),
            pltpu.VMEM((64, 1024), BF),
            pltpu.VMEM((1024, 3072), BF),
            pltpu.VMEM((1024, 1024), BF),
            pltpu.VMEM((256, 1024), BF),
            pltpu.VMEM((256, 1024), BF),
            pltpu.VMEM((768, 2048), BF),
            pltpu.VMEM((256, 1024), BF),
            pltpu.VMEM((256, 768), F32),
            pltpu.VMEM((256, 1024), F32),
            pltpu.VMEM((256, 1024), F32),
            pltpu.VMEM((256, 1024), F32),
            dma((8,)), dma((3,)), dma((n,)), dma((n,)), dma((2,)), dma((2,)), dma((3,)), dma, dma, dma((8,)),
            dma((3,)), dma((3,)),
        ],
        compiler_params=pltpu.CompilerParams(collective_id=0, has_side_effects=True, vmem_limit_bytes=62 * 2**20),
    )(up, query_w, key_w, value_w, embed, count, gain, qkv, enc_out)


def second_kernel(
    hidden, marks_row, marks_col, counts, gain, weights_hbm, out_w, down_t,
    out,
    w, own, w2, ones, parts, part_relay, arrived, share, pooled, latent, scaled, acc, kv, kv_all, query, mx, tot, mix, attn,
    far, relay_r, relay_l, to_right, to_left, arr_r, arr_l, lat_out, downs, down_relay, down_in, down_share, patch,
    lead, lead_in, trail, trail_in,
    w_sem, p_send, p_recv, s_send, s_recv, l_send, l_recv, f_send, f_recv, z_send, z_recv, x_send, x_recv,
    o_send, o_recv, d_send, d_recv, e_send, e_recv, lead_send, lead_recv, trail_send, trail_recv,
    own_sem, g_send, g_recv,
):
    ctx, tp, dp = position()
    h, x = ctx // 4, ctx % 4
    load = pltpu.make_async_copy(weights_hbm, w, w_sem)
    load.start()
    loads = [pltpu.make_async_copy(out_w, own.at[pl.ds(0, 512)], own_sem.at[0])]
    loads += [
        pltpu.make_async_copy(down_t.at[:, pl.ds(256 * i, 256)], own.at[pl.ds(512 + 64 * i, 64)], own_sem.at[1 + i])
        for i in range(4)
    ]
    for c in loads:
        c.start()
    gather = Gather(own, w2, g_send, g_recv)
    link = gather_links(ctx, tp, dp)
    tps = [(ctx, (tp + i) % 4, dp) for i in (1, 2, 3)]
    up_y, down_y = tps[0], tps[2]
    zs = [(((h + i) % 4) * 4 + x, tp, dp) for i in (1, 3)]
    right, left = (h * 4 + (x + 1) % 4, tp, dp), (h * 4 + (x + 3) % 4, tp, dp)
    next_first = ((ctx + 1) % 16, tp * 0, dp)
    before_all = [((ctx + 15) % 16, t, dp) for t in range(4)]
    barrier = pltpu.get_barrier_semaphore()

    def greet(devices):
        for device in devices:
            pl.semaphore_signal(barrier, inc=1, device_id=device, device_id_type=MESH)

    greet(tps + zs + [right, left, next_first] + [link[name] for name in ("E", "I", "D")])

    @pl.when(tp == 0)
    def _():
        greet(before_all)

    def dot(a, b):
        return jnp.dot(a, b, preferred_element_type=F32)

    def iota(shape, dim):
        return lax.broadcasted_iota(jnp.int32, shape, dim).astype(F32)

    ones[...] = jnp.ones_like(ones)
    r256, c256 = iota((256, 256), 0), iota((256, 256), 1)
    c4 = [counts[t].astype(F32) for t in range(4)]
    offset = jnp.zeros((8, 128), F32)
    for t in range(4):
        offset = offset + jnp.where(tp > t, c4[t], F32(0.0))
    group = c4[0] + c4[1] + c4[2] + c4[3]
    offset, group_one = offset[0:1, 0:1], group[0:1, 0:1]
    run_row = dot(marks_row[...], (r256 <= c256).astype(BF))
    run_col = dot((r256 >= c256).astype(BF), marks_col[...])[:, 0:1]
    slot_row = run_row[0:1] + offset - 1.0
    slot_col = run_col + offset - 1.0
    place = (r256 == slot_row).astype(BF)
    mass = dot(place, hidden[...])
    number = dot(place, ones[...])
    for t in range(4):
        parts[t, :, pl.ds(0, 1024)] = mass[64 * t : 64 * t + 64].astype(BF)
        parts[t, :, pl.ds(1024, 128)] = number[64 * t : 64 * t + 64].astype(BF)
    leading = (run_row == 0.0).astype(BF)
    lead[:, pl.ds(0, 1024)] = dot(leading, hidden[...])
    lead[:, pl.ds(1024, 128)] = dot(leading, ones[...])

    pl.semaphore_wait(barrier, 11 + 4 * (tp == 0).astype(jnp.int32))

    leads = [remote(lead.at[pl.ds(0, 8)], lead_in, lead_send.at[t], lead_recv, before_all[t]) for t in range(4)]

    @pl.when(tp == 0)
    def _():
        for c in leads:
            c.start()

    opposite, above, below = (tp + 2) % 4, (tp + 1) % 4, (tp + 3) % 4
    half_a, half_b = pl.ds(0, 32), pl.ds(32, 32)

    def scatter(src, relay, dst, send, recv):
        return [
            remote(src.at[opposite, half_a], relay.at[0], send.at[0], recv.at[0], up_y),
            remote(src.at[opposite, half_b], relay.at[1], send.at[1], recv.at[1], down_y),
            remote(src.at[above], dst.at[0], send.at[2], recv.at[2], up_y),
            remote(src.at[below], dst.at[1], send.at[3], recv.at[3], down_y),
        ]

    def pass_on(src, relay, copies):
        copies[0].wait_recv()
        src[above, half_a] = (src[above, half_a].astype(F32) + relay[0].astype(F32)).astype(BF)
        copies[2].start()
        copies[1].wait_recv()
        src[below, half_b] = (src[below, half_b].astype(F32) + relay[1].astype(F32)).astype(BF)
        copies[3].start()

    def gathered(src, dst, copies):
        copies[2].wait_recv()
        copies[3].wait_recv()
        return src[tp].astype(F32) + dst[0].astype(F32) + dst[1].astype(F32)

    def spread(src, dst, send, recv):
        lower, upper = dst.at[below, half_a], dst.at[above, half_b]
        return [
            remote(src, dst.at[tp], send.at[0], recv.at[0], up_y),
            remote(src, dst.at[tp], send.at[1], recv.at[1], down_y),
            remote(lower, lower, send.at[2], recv.at[2], up_y),
            remote(upper, upper, send.at[3], recv.at[3], down_y),
        ]

    def spread_rest(copies):
        for i in (0, 1):
            copies[i].wait_recv()
            copies[2 + i].start()
        for i in (2, 3):
            copies[i].wait_recv()

    first = scatter(parts, part_relay, arrived, p_send, p_recv)
    for c in first[:2]:
        c.start()
    for c in loads:
        c.wait()
    gather.until(0.0)
    w2[pl.ds(h, 1), pl.ds(x, 1)] = own[...][None, None]
    pass_on(parts, part_relay, first)
    gather.until(7.0)
    sums = gathered(parts, arrived, first)
    leads[0].wait_recv()
    my_row = iota((64, 1152), 0) + (64 * tp).astype(F32)
    sums = sums + jnp.where(my_row == group_one - 1.0, lead_in[0:1], F32(0.0))
    share[...] = (sums[:, :1024] / jnp.maximum(sums[:, 1024:1025], 1.0)).astype(BF)
    second = spread(share, pooled, s_send, s_recv)
    for c in second[:2]:
        c.start()
    pooled[pl.ds(tp, 1)] = share[...][None]
    load.wait()
    gather.until(14.0)
    spread_rest(second)

    def columns(t, i):
        return pl.ds(pl.multiple_of(1024 * t + 256 * i, 256), 256)

    def sent(i):
        block = latent.at[:, columns(tp, i)]
        return [
            remote(block, block, l_send.at[i], l_recv.at[i], up_y),
            remote(block, block, l_send.at[4 + i], l_recv.at[4 + i], down_y),
        ]

    def passed(i):
        block = latent.at[:, columns((tp + 3) % 4 if i < 2 else (tp + 1) % 4, i)]
        return remote(block, block, f_send.at[i], f_recv.at[i], up_y if i < 2 else down_y)

    all_pooled = pooled[...].reshape(256, 1024)
    for i in range(4):
        block = w[:, :, pl.ds(64 * i, 64), :].reshape(1024, 256)
        latent[:, columns(tp, i)] = dot(all_pooled, block).astype(BF)
        for c in sent(i):
            c.start()
    gather.until(18.0)

    def contract(t, i, fresh=False):
        values = latent[:, columns(t, i)].astype(F32)
        inputs = (values * gain[:, columns(t, i)]).astype(BF)
        power = jnp.sum(values * values, axis=-1, keepdims=True)
        scaled[...] = power if fresh else scaled[...] + power
        for b in range(3):
            term = dot(inputs, w[t, i, pl.ds(256 + 256 * b, 256), :])
            acc[b] = term if fresh else acc[b] + term

    for i in range(4):
        contract(tp, i, i == 0)
        gather.until(19.5 + 1.5 * i)
    for i in range(4):
        remote(latent.at[:, columns(tp, i)], latent.at[:, columns(tp, i)], l_send.at[i], l_recv.at[i], up_y).wait_recv()
        if i < 2:
            passed(i).start()
        remote(latent.at[:, columns(tp, i)], latent.at[:, columns(tp, i)], l_send.at[4 + i], l_recv.at[4 + i], down_y).wait_recv()
        if i >= 2:
            passed(i).start()
        contract((tp + 3) % 4, i)
        contract((tp + 1) % 4, i)
        gather.until(26.0 + 2.0 * i)
    for i in (0, 2, 1, 3):
        passed(i).wait_recv()
        contract((tp + 2) % 4, i)
    gather.until(35.0)
    scale = lax.rsqrt(scaled[...] * F32(1.0 / 4096.0) + EPS)
    kv[pl.ds(0, 256)] = (acc[2] * scale).astype(BF)
    kv[pl.ds(256, 16)] = jnp.broadcast_to(group_one, (16, 256)).astype(BF)

    low_rows, high_rows = pl.ds(0, 128), pl.ds(128, 144)
    z_low, z_high = kv_all.at[(h + 3) % 4, x, low_rows], kv_all.at[(h + 1) % 4, x, high_rows]
    z_copies = [remote(kv, kv_all.at[h, x], z_send.at[i], z_recv.at[i], zs[i]) for i in range(2)]
    z_copies.append(remote(z_low, z_low, z_send.at[2], z_recv.at[2], zs[0]))
    z_copies.append(remote(z_high, z_high, z_send.at[3], z_recv.at[3], zs[1]))
    for c in z_copies[:2]:
        c.start()

    def across(j, dz):
        z = (h + dz) % 4
        src = kv if dz == 0 else kv_all.at[z, x]
        lower, upper = pl.ds(0, 128), pl.ds(128, 144)
        a, b = (x + 3) % 4, (x + 1) % 4
        return [
            remote(src, kv_all.at[z, x], x_send.at[4 * j], x_recv.at[4 * j], right),
            remote(src, kv_all.at[z, x], x_send.at[4 * j + 1], x_recv.at[4 * j + 1], left),
            remote(kv_all.at[z, a, lower], kv_all.at[z, a, lower], x_send.at[4 * j + 2], x_recv.at[4 * j + 2], right),
            remote(kv_all.at[z, b, upper], kv_all.at[z, b, upper], x_send.at[4 * j + 3], x_recv.at[4 * j + 3], left),
        ]

    turns = (0, 3, 1, 2)
    sets = [across(j, dz) for j, dz in enumerate(turns)]
    sets[0][0].start()
    sets[0][1].start()
    kv_all[pl.ds(h, 1), pl.ds(x, 1)] = kv[...][None, None]
    for head in range(4):
        q = acc[head // 2][:, 128 * (head % 2) : 128 * (head % 2) + 128] * scale
        query[pl.ds(256 * head, 256)] = q.astype(BF)

    shrink = F32(1.0) / jnp.sqrt(F32(HEAD_SIZE))

    def attend(dz, dx, fresh=False):
        z, xx = (h + dz) % 4, (x + dx) % 4
        other = z * 4 + xx

        @pl.when(other <= ctx)
        def _():
            keys = kv_all[z, xx, pl.ds(0, 256), pl.ds(0, 128)]
            values = kv_all[z, xx, pl.ds(0, 256), pl.ds(128, 128)]
            limit = kv_all[z, xx, pl.ds(256, 16), :][0:1].astype(F32)
            bias = jnp.where(c256[0:1] < limit, F32(0.0), F32(-1e30))
            if fresh:
                causal = jnp.where(c256 <= r256, F32(0.0), F32(-1e30))
                bias = bias + jnp.concatenate([causal, causal], axis=0)

            def two_heads(i, carry):
                rows = pl.ds(pl.multiple_of(512 * i, 512), 512)
                s = nt(query[rows], keys) * shrink + bias
                peak = jnp.max(s, axis=-1, keepdims=True)
                if not fresh:
                    old = mx[rows]
                    peak = jnp.maximum(peak, old)
                e = jnp.exp(s - peak)
                total = jnp.sum(e, axis=-1, keepdims=True)
                mixed = dot(e.astype(BF), values)
                if not fresh:
                    fade = jnp.exp(old - peak)
                    total = total + tot[rows] * fade
                    mixed = mixed + mix[rows] * fade
                mx[rows] = peak
                tot[rows] = total
                mix[rows] = mixed
                return carry

            lax.fori_loop(0, 2, two_heads, 0)

    def along(j):
        sets[j][0].start()
        sets[j][1].start()

    def turn(j):
        for i in (0, 1):
            sets[j][i].wait_recv()
            sets[j][i + 2].start()

    attend(0, 0, True)
    gather.until(38.0)
    for i in (0, 1):
        z_copies[i].wait_recv()
        z_copies[i + 2].start()
        along(i + 1)
    turn(0)
    attend(3, 0)
    attend(1, 0)
    attend(0, 3)
    z_copies[2].wait_recv()
    z_copies[3].wait_recv()
    along(3)
    attend(0, 1)
    turn(1)
    gather.until(1000.0)
    attend(3, 3)
    turn(2)
    attend(3, 1)
    attend(2, 0)
    attend(1, 3)
    turn(3)
    attend(1, 1)
    attend(2, 3)
    attend(2, 1)
    for j in range(4):
        for i in (2, 3):
            sets[j][i].wait_recv()
        attend(turns[j], 2)
    for head in range(4):
        rows = pl.ds(256 * head, 256)
        attn[:, pl.ds(128 * head, 128)] = (mix[rows] / tot[rows]).astype(BF)

    def part(t, i):
        return dot(attn[...], w2[t, i, pl.ds(0, 512), :])

    def block(i):
        return pl.ds(256 * i, 256)

    low, high = pl.ds(0, 128), pl.ds(128, 128)
    for i in range(4):
        far[:, block(i)] = part(opposite, i).astype(BF)
    o_copies = [
        remote(far.at[low], relay_r, o_send.at[0], o_recv.at[0], up_y),
        remote(far.at[high], relay_l, o_send.at[1], o_recv.at[1], down_y),
        remote(to_right, arr_r, o_send.at[2], o_recv.at[2], up_y),
        remote(to_left, arr_l, o_send.at[3], o_recv.at[3], down_y),
    ]
    o_copies[0].start()
    o_copies[1].start()
    for i in range(4):
        acc_r = part(above, i)
        if i == 0:
            o_copies[0].wait_recv()
        to_right[low, block(i)] = (acc_r[:128] + relay_r[:, block(i)].astype(F32)).astype(BF)
        to_right[high, block(i)] = acc_r[128:].astype(BF)
    o_copies[2].start()
    for i in range(4):
        acc_l = part(below, i)
        if i == 0:
            o_copies[1].wait_recv()
        to_left[low, block(i)] = acc_l[:128].astype(BF)
        to_left[high, block(i)] = (acc_l[128:] + relay_l[:, block(i)].astype(F32)).astype(BF)
    o_copies[3].start()
    o_copies[2].wait_recv()
    o_copies[3].wait_recv()
    total_down = jnp.zeros((256, 1024), F32)
    for i in range(4):
        value = part(tp, i) + latent[:, columns(tp, i)].astype(F32)
        value = value + arr_r[:, block(i)].astype(F32) + arr_l[:, block(i)].astype(F32)
        lat_out[:, block(i)] = value.astype(BF)
    for i in range(4):
        down = w2[:, :, pl.ds(512 + 64 * i, 64), :].reshape(1024, 256)
        total_down = total_down + nt(lat_out[:, block(i)], down)
    for t in range(4):
        downs[t] = total_down[64 * t : 64 * t + 64].astype(BF)
    third = scatter(downs, down_relay, down_in, d_send, d_recv)
    for c in third[:2]:
        c.start()
    pass_on(downs, down_relay, third)
    sums = gathered(downs, down_in, third)
    down_share[...] = sums.astype(BF)
    final = (iota((16, 64), 1) + (64 * tp).astype(F32) == group_one - 1.0).astype(BF)
    trail[...] = dot(final, down_share[...]).astype(BF)
    fourth = spread(down_share, patch, e_send, e_recv)
    for c in fourth[:2]:
        c.start()
    trail_copies = [remote(trail, trail_in.at[t], trail_send, trail_recv.at[t], next_first) for t in range(4)]
    for t in range(4):

        @pl.when(tp == t)
        def _():
            trail_copies[t].start()

    patch[pl.ds(tp, 1)] = down_share[...][None]
    spread_rest(fourth)
    patch_out = patch[...].reshape(256, 1024)
    result = hidden[...].astype(F32) + dot((c256 == slot_col).astype(BF), patch_out)
    out[...] = result.astype(BF)

    @pl.when(tp == 0)
    def _():
        row = jnp.zeros((1, 1024), F32)
        for t in range(4):
            trail_copies[t].wait_recv()
            row = row + trail_in[t][0:1].astype(F32)
        out[...] = (out[...].astype(F32) + jnp.where(run_col == 0.0, row, F32(0.0))).astype(BF)

    trail_copies[0].wait_send()

    @pl.when(tp == 0)
    def _():
        for c in leads:
            c.wait_send()

    for c in first + second + third + fourth + z_copies + o_copies:
        c.wait_send()
    for i in range(4):
        for c in sent(i):
            c.wait_send()
        passed(i).wait_send()
    for group_of in sets:
        for c in group_of:
            c.wait_send()
    gather.drain()


def second_stage(hidden, marks_row, marks_col, counts, gain, weights, out_w, down_t):
    anywhere = pl.BlockSpec(memory_space=pl.ANY)
    vmem = pl.BlockSpec(memory_space=pltpu.VMEM)
    dma = pltpu.SemaphoreType.DMA

    n = len(PLANS[SECOND][1])

    def v(*shape, kind=BF):
        return pltpu.VMEM(shape, kind)

    return pl.pallas_call(
        second_kernel,
        out_shape=jax.ShapeDtypeStruct(hidden.shape, BF),
        in_specs=[vmem] * 5 + [anywhere] * 3,
        out_specs=vmem,
        scratch_shapes=[
            v(4, 4, FIRST, 256), v(SECOND, 256), v(4, 4, SECOND, 256), v(256, 128), v(4, 64, 1152), v(2, 32, 1152), v(2, 64, 1152), v(64, 1024), v(4, 64, 1024),
            v(256, 4096), v(256, 1, kind=F32), v(3, 256, 256, kind=F32), v(272, 256), v(4, 4, 272, 256),
            v(1024, 128), v(1024, 1, kind=F32), v(1024, 1, kind=F32), v(1024, 128, kind=F32), v(256, 512),
            v(256, 1024), v(128, 1024), v(128, 1024), v(256, 1024), v(256, 1024), v(256, 1024), v(256, 1024),
            v(256, 1024), v(4, 64, 1024), v(2, 32, 1024), v(2, 64, 1024), v(64, 1024), v(4, 64, 1024),
            v(16, 1152, kind=F32), v(8, 1152, kind=F32), v(16, 1024), v(4, 16, 1024),
            dma, dma((4,)), dma((4,)), dma((4,)), dma((4,)), dma((8,)), dma((8,)), dma((4,)), dma((4,)),
            dma((4,)), dma((4,)), dma((16,)), dma((16,)), dma((4,)), dma((4,)), dma((4,)), dma((4,)),
            dma((4,)), dma((4,)), dma((4,)), dma, dma, dma((4,)),
            dma((5,)), dma((n,)), dma((n,)),
        ],
        compiler_params=pltpu.CompilerParams(collective_id=1, has_side_effects=True, vmem_limit_bytes=62 * 2**20),
    )(hidden, marks_row, marks_col, counts, gain, weights, out_w, down_t)


def local(
    byte_embed, patch_start, enc_gain, enc_qkv, enc_out, up_proj, lat_gain, query_proj, key_proj,
    value_matrix, out_proj, down_proj,
):
    local_count = jnp.sum(patch_start)
    whole, hidden, counts = first_stage(
        up_proj, query_proj, key_proj, value_matrix, byte_embed,
        jnp.full((8, 128), local_count, jnp.int32), enc_gain[None, :], enc_qkv, enc_out,
    )
    marks = patch_start.astype(BF)
    marks_row = jnp.broadcast_to(marks[None, :], (16, 256))
    marks_col = jnp.broadcast_to(marks[:, None], (256, 128))
    return second_stage(hidden, marks_row, marks_col, counts, lat_gain[None, :], whole, out_proj, down_proj.T)


def solution(mesh):
    placed = (
        P(("dp", "ctx", "tp"), None), P(("dp", "ctx", "tp")), P(), P(), P(), P("ctx", "tp"), P(),
        P("ctx", "tp"), P("ctx", "tp"), P("ctx", "tp"), P("tp", "ctx"), P("tp", "ctx"),
    )
    return jax.shard_map(
        local, mesh=mesh, in_specs=placed, out_specs=P(("dp", "ctx", "tp"), None), check_vma=False
    )
```

```python
import heapq

import jax
import jax.numpy as jnp
from jax import lax
from jax.experimental import pallas as pl
from jax.experimental.pallas import tpu as pltpu
from jax.sharding import PartitionSpec as P

BH = 16
HB = 64
HEAD_SIZE = 128
WIN = 512
EPS = 1e-05
MESH = pl.DeviceIdType.MESH
BF = jnp.bfloat16
F32 = jnp.float32
FIRST, SECOND = 1024, 768


def gather_plan(whole_rows, rate=46.6e3, latency=2.0):
    sizes = {"A": whole_rows // 4, "B": whole_rows // 4}
    free = {link: 0.0 for link in ("E", "I", "X+", "X-", "D")}
    heap, order, sends, halves = [], [], [], {}

    def send(now, kind, dz, dx, half, link, batch):
        rows = sizes[kind] // (1 if half is None else 2)
        end = max(now, free[link]) + rows * 512 / (650e3 if link == "D" else rate)
        free[link] = end
        sends.append((kind, dz, dx, half, link))
        batch.append(len(sends) - 1)
        heapq.heappush(heap, (end + (1.0 if link == "D" else latency), len(sends) - 1))

    def have(now, kind, dz, dx, batch):
        if kind == "A" and dx == 0:
            if dz == 0:
                send(now, "A", 0, 0, None, "E", batch)
            elif dz == 1:
                send(now, "A", 1, 0, None, "I", batch)
            elif dz == -1:
                send(now, "A", -1, 0, "other", "E", batch)
            send(now, "A", dz, 0, None, "X+", batch)
            send(now, "A", dz, 0, None, "X-", batch)
        elif kind == "A" and dx == -1:
            send(now, "A", dz, -1, 0, "X+", batch)
        elif kind == "A" and dx == 1:
            send(now, "A", dz, 1, 1, "X-", batch)
        elif kind == "B" and dz == 0:
            if dx == 0:
                send(now, "B", 0, 0, None, "X+", batch)
                send(now, "B", 0, 0, None, "X-", batch)
            elif dx == -1:
                send(now, "B", 0, -1, 0, "X+", batch)
            elif dx == 1:
                send(now, "B", 0, 1, 1, "X-", batch)
            send(now, "B", 0, dx, None, "E", batch)
        elif kind == "B" and dz == 1:
            send(now, "B", 1, dx, None, "I", batch)
        elif kind == "B" and dz == -1:
            send(now, "B", -1, dx, "other", "E", batch)
        if (dz, dx) != (0, 0):
            send(now, kind, dz, dx, None, "D", batch)

    first = []
    have(0.0, "A", 0, 0, first)
    have(0.0, "B", 0, 0, first)
    order.append((0.0, None, first))
    while heap:
        now, k = heapq.heappop(heap)
        kind, dz, dx, half, link = sends[k]
        batch = []
        if link != "D":
            if link == "E":
                dz = 1 if dz == 0 else 2
            elif link == "I":
                dz = {1: -1, 2: 2}[dz]
            elif link == "X+":
                dx = {0: -1, -1: 2}[dx]
            else:
                dx = {0: 1, 1: 2}[dx]
            if half is None:
                have(now, kind, dz, dx, batch)
            else:
                key = (kind, dz, dx)
                halves[key] = halves.get(key, 0) + 1
                if link == "E":
                    send(now, kind, 2, dx, "mine", "I", batch)
                if halves[key] == 2:
                    have(now, kind, dz, dx, batch)
        order.append((now, k, batch))
    return order, sends


PLANS = {FIRST: gather_plan(FIRST), SECOND: gather_plan(SECOND, 38e3, 2.5)}


def enter(devices):
    barrier = pltpu.get_barrier_semaphore()
    for device in devices:
        pl.semaphore_signal(barrier, inc=1, device_id=device, device_id_type=MESH)
    pl.semaphore_wait(barrier, len(devices))


def position():
    return lax.axis_index("ctx"), lax.axis_index("tp"), lax.axis_index("dp")


def remote(src, dst, send, recv, device):
    return pltpu.make_async_remote_copy(
        src_ref=src, dst_ref=dst, send_sem=send, recv_sem=recv, device_id=device, device_id_type=MESH
    )


def gather_links(ctx, tp, dp):
    h, x, lo, core = ctx // 4, ctx % 4, dp // 2, dp % 2
    way = 2 * lo - 1
    turned = (1 - lo) * 2 + core
    return {
        "E": (((h + way + 4) % 4) * 4 + x, tp, turned),
        "I": (ctx, tp, turned),
        "X+": (h * 4 + (x + 1) % 4, tp, dp),
        "X-": (h * 4 + (x + 3) % 4, tp, dp),
        "D": (ctx, tp, lo * 2 + 1 - core),
    }


class Gather:
    def __init__(self, own, whole, send, recv):
        self.own, self.whole, self.send, self.recv = own, whole, send, recv
        self.order, self.sends = PLANS[own.shape[0]]
        self.at = 0

    def copy(self, k):
        ctx, tp, dp = position()
        h, x, lo, core = ctx // 4, ctx % 4, dp // 2, dp % 2
        kind, dz, dx, half, where = self.sends[k]
        rows = self.own.shape[0] // 4
        base = core * 2 * rows + (0 if kind == "A" else rows)
        if half is not None:
            rows = rows // 2
            base = base + {"mine": lo, "other": 1 - lo}.get(half, half) * rows
        part = pl.ds(pl.multiple_of(base, 16), rows)
        piece = self.whole.at[(h + dz * (2 * lo - 1) + 8) % 4, (x + dx + 4) % 4, part]
        device = gather_links(ctx, tp, dp)[where]
        src = self.own.at[part] if (dz, dx) == (0, 0) else piece
        return remote(src, piece, self.send.at[k], self.recv.at[k], device)

    def until(self, time):
        while self.at < len(self.order) and self.order[self.at][0] <= time:
            _, k, batch = self.order[self.at]
            if k is not None:
                self.copy(k).wait_recv()
            for s in batch:
                self.copy(s).start()
            self.at += 1

    def drain(self):
        for k in range(len(self.sends)):
            self.copy(k).wait_send()


def normal(rows, gain):
    floats = rows.astype(F32)
    return (floats * lax.rsqrt(jnp.mean(floats * floats, axis=-1, keepdims=True) + EPS) * gain).astype(BF)


def nt(a, b):
    return lax.dot_general(a, b, (((1,), (1,)), ((), ())), preferred_element_type=F32)


def first_kernel(
    up, query_w, key_w, value_w, embed, count, gain, qkv_hbm, out_hbm,
    whole, hidden, counts,
    own, halo, relay, qkv, enc_out, normed, query, keyval, mixed, bias, peaks_of, totals_of, sums_of,
    own_sem, w_sem, g_send, g_recv, h_send, h_recv, r_send, r_recv, x_send, x_recv, c_send, c_recv,
):
    ctx, tp, dp = position()
    h, x = ctx // 4, ctx % 4
    link = gather_links(ctx, tp, dp)
    loads = [pltpu.make_async_copy(up.at[:, pl.ds(256 * i, 256)], own.at[pl.ds(64 * i, 64)], own_sem.at[i]) for i in range(4)]
    loads += [
        pltpu.make_async_copy(query_w.at[:, pl.ds(256 * i, 256)], own.at[pl.ds(256 + 256 * i, 256)], own_sem.at[4 + i])
        for i in range(2)
    ]
    loads.append(pltpu.make_async_copy(key_w, own.at[pl.ds(768, 256), pl.ds(0, 128)], own_sem.at[6]))
    loads.append(pltpu.make_async_copy(value_w, own.at[pl.ds(768, 256), pl.ds(128, 128)], own_sem.at[7]))
    for load in loads:
        load.start()
    weights = [pltpu.make_async_copy(qkv_hbm, qkv, w_sem.at[0]), pltpu.make_async_copy(out_hbm, enc_out, w_sem.at[1])]
    for load in weights:
        load.start()

    gather = Gather(own, whole, g_send, g_recv)
    last = (tp == 3).astype(jnp.int32)
    zero = (tp == 0).astype(jnp.int32)
    following = ((ctx + last) % 16, (tp + 1) % 4, dp)
    previous = ((ctx - zero + 16) % 16, (tp + 3) % 4, dp)
    tps = [(ctx, (tp + i) % 4, dp) for i in (1, 2, 3)]
    over = ((((h + 1) % 4) * 4), tp * 0, dp)
    under = [((((h + 3) % 4) * 4 + j), t, dp) for t in (2, 3) for j in range(4)]
    row_mates = [(h * 4 + j, tp, dp) for j in range(3)]
    origin = (h * 4 + 3, tp, dp)
    upper = tp >= 2
    sends_over = (x == 3) & upper
    relays = (x < 3) & upper
    takes_over = (x == 0) & (tp == 0)
    crossing = (x == 3) & (tp == 3)

    barrier = pltpu.get_barrier_semaphore()

    def greet(devices):
        for device in devices:
            pl.semaphore_signal(barrier, inc=1, device_id=device, device_id_type=MESH)

    greet([link[name] for name in ("E", "I", "X+", "X-", "D")] + [following, previous] + tps)

    @pl.when(sends_over)
    def _():
        greet(row_mates + [over])

    @pl.when(relays)
    def _():
        greet([origin, over])

    @pl.when(takes_over)
    def _():
        greet(under)

    more = 4 * sends_over.astype(jnp.int32) + 2 * relays.astype(jnp.int32) + 8 * takes_over.astype(jnp.int32)
    pl.semaphore_wait(barrier, 10 + more)

    one = remote(embed, halo.at[1], h_send.at[0], h_recv.at[0], following)
    two = remote(halo.at[1], halo.at[0], h_send.at[1], h_recv.at[1], following)
    to_relay = [remote(embed.at[pl.ds(64 * j, 64)], relay, r_send.at[j], r_recv, row_mates[j]) for j in range(3)]

    def over_copy(t, j):
        src = embed.at[pl.ds(192, 64)] if j == 3 else relay
        return remote(src, halo.at[t - 2, pl.ds(64 * j, 64)], x_send, x_recv.at[4 * (t - 2) + j], over)

    def each_over(action, columns):
        for t in (2, 3):
            for j in columns:

                @pl.when((tp == t) & (x == j))
                def _():
                    action(over_copy(t, j))

    @pl.when(sends_over)
    def _():
        for c in to_relay:
            c.start()

    each_over(lambda c: c.start(), (3,))

    @pl.when(jnp.logical_not(crossing))
    def _():
        one.start()

    for i, device in enumerate(tps):
        remote(count, counts.at[tp], c_send.at[i], c_recv.at[i], device).start()
    counts[pl.ds(tp, 1)] = count[...][None]

    def first_sends():
        for load in loads:
            load.wait()
        gather.until(0.0)

    def project(block, rows, columns):
        normed[...] = normal(rows, gain[...])

        def tile(i, carry):
            at = pl.multiple_of(i * 256, 256)
            piece = jnp.dot(normed[...], qkv[:, pl.ds(1024 + at, 256)], preferred_element_type=F32).astype(BF)
            keyval[pl.ds(256 * block, 256), pl.ds(at, 256)] = piece
            return carry

        lax.fori_loop(0, 8, tile, 0)
        if columns:

            def query_tile(i, carry):
                at = pl.multiple_of(i * 256, 256)
                piece = jnp.dot(normed[...], qkv[:, pl.ds(at, 256)], preferred_element_type=F32)
                query[:, pl.ds(at, 256)] = (piece.astype(BF).astype(F32) * 0.125).astype(BF)
                return carry

            lax.fori_loop(0, 4, query_tile, 0)

    def own_part():
        r = lax.broadcasted_iota(jnp.int32, (256, 768), 0)
        c = lax.broadcasted_iota(jnp.int32, (256, 768), 1)
        floor = 512 - 256 * (ctx * 4 + tp)
        bias[...] = jnp.where((c <= r + 512) & (c > r) & (c >= floor), F32(0.0), F32(-1e30))
        weights[0].wait()
        project(2, embed[...], True)

    def relay_part():
        @pl.when(relays)
        def _():
            remote(embed.at[pl.ds(0, 64)], relay, r_send.at[0], r_recv, origin).wait_recv()

        each_over(lambda c: c.start(), (0, 1, 2))

    def near_part():
        @pl.when(jnp.logical_not(takes_over))
        def _():
            one.wait_recv()

        @pl.when(takes_over)
        def _():
            for j in range(4):
                over_copy(3, j).wait_recv()

        @pl.when(jnp.logical_not(crossing))
        def _():
            two.start()

        project(1, halo[1], False)

    def far_part():
        @pl.when(jnp.logical_not(takes_over))
        def _():
            two.wait_recv()

        @pl.when(takes_over)
        def _():
            for j in range(4):
                over_copy(2, j).wait_recv()

        project(0, halo[0], False)

    lanes = lax.broadcasted_iota(jnp.int32, (256, 128), 1)

    def attend(block, pair, carry):
        at = pl.ds(pl.multiple_of(128 * pair, 128), 128)
        rows = pl.ds(256 * block, 256)
        both = query[:, at]
        k = keyval[rows, at]
        v = keyval[rows, pl.ds(pl.multiple_of(1024 + 128 * pair, 128), 128)]
        peaks, totals, outs, fades = [], [], [], []
        for side in range(2):
            q = jnp.where((lanes < 64) == (side == 0), both, jnp.zeros_like(both))
            s = nt(q, k) + bias[:, rows]
            peak = jnp.max(s, axis=-1, keepdims=True)
            if block != 2:
                old = peaks_of[:, at][:, 64 * side : 64 * side + 1]
                peak = jnp.maximum(peak, old)
                fades.append(jnp.exp(old - peak))
            e = jnp.exp(s - peak)
            peaks.append(peak)
            totals.append(jnp.sum(e, axis=-1, keepdims=True))
            outs.append(jnp.dot(e.astype(BF), v, preferred_element_type=F32))
        first = lanes < 64
        total, out = jnp.where(first, *totals), jnp.where(first, *outs)
        if block != 2:
            fade = jnp.where(first, *fades)
            total = total + totals_of[:, at] * fade
            out = out + sums_of[:, at] * fade
        if block == 0:
            mixed[:, at] = (out / total).astype(BF)
        else:
            peaks_of[:, at] = jnp.where(first, *peaks)
            totals_of[:, at] = total
            sums_of[:, at] = out
        return carry

    def attend_block(block, times):
        for i, time in enumerate(times):
            n = 8 // len(times)
            lax.fori_loop(n * i, n * i + n, lambda pair, carry: attend(block, pair, carry), 0)
            gather.until(time)

    def finish():
        weights[1].wait()

        def tile(i, carry):
            at = pl.ds(pl.multiple_of(i * 256, 256), 256)
            piece = jnp.dot(mixed[...], enc_out[:, at], preferred_element_type=F32)
            hidden[:, at] = (embed[:, at].astype(F32) + piece).astype(BF)
            return carry

        lax.fori_loop(0, 4, tile, 0)

    own_part()
    relay_part()
    first_sends()
    keep = pltpu.make_async_copy(own, whole.at[h, x], w_sem.at[2])
    keep.start()
    attend_block(2, (2.0, 4.0, 6.0, 8.0))
    near_part()
    gather.until(10.0)
    attend_block(1, (13.0, 16.0, 19.0, 22.0))
    far_part()
    gather.until(26.0)
    attend_block(0, (28.0, 30.0, 33.0, 36.0))
    finish()
    gather.until(1000.0)
    keep.wait()

    @pl.when(jnp.logical_not(crossing))
    def _():
        one.wait_send()
        two.wait_send()

    @pl.when(sends_over)
    def _():
        for c in to_relay:
            c.wait_send()

    each_over(lambda c: c.wait_send(), (0, 1, 2, 3))
    for i, device in enumerate(tps):
        remote(count, counts.at[tp], c_send.at[i], c_recv.at[i], device).wait()
    gather.drain()


def first_stage(up, query_w, key_w, value_w, embed, count, gain, qkv, enc_out):
    anywhere = pl.BlockSpec(memory_space=pl.ANY)
    vmem = pl.BlockSpec(memory_space=pltpu.VMEM)
    n = len(PLANS[FIRST][1])
    dma = pltpu.SemaphoreType.DMA
    return pl.pallas_call(
        first_kernel,
        out_shape=(
            jax.ShapeDtypeStruct((4, 4, FIRST, 256), BF),
            jax.ShapeDtypeStruct(embed.shape, BF),
            jax.ShapeDtypeStruct((4, 8, 128), jnp.int32),
        ),
        in_specs=[anywhere] * 4 + [vmem] * 3 + [anywhere] * 2,
        out_specs=(anywhere, vmem, vmem),
        scratch_shapes=[
            pltpu.VMEM((FIRST, 256), BF),
            pltpu.VMEM((2, 256, 1024), BF),
            pltpu.VMEM((64, 1024), BF),
            pltpu.VMEM((1024, 3072), BF),
            pltpu.VMEM((1024, 1024), BF),
            pltpu.VMEM((256, 1024), BF),
            pltpu.VMEM((256, 1024), BF),
            pltpu.VMEM((768, 2048), BF),
            pltpu.VMEM((256, 1024), BF),
            pltpu.VMEM((256, 768), F32),
            pltpu.VMEM((256, 1024), F32),
            pltpu.VMEM((256, 1024), F32),
            pltpu.VMEM((256, 1024), F32),
            dma((8,)), dma((3,)), dma((n,)), dma((n,)), dma((2,)), dma((2,)), dma((3,)), dma, dma, dma((8,)),
            dma((3,)), dma((3,)),
        ],
        compiler_params=pltpu.CompilerParams(collective_id=0, has_side_effects=True, vmem_limit_bytes=62 * 2**20),
    )(up, query_w, key_w, value_w, embed, count, gain, qkv, enc_out)


def second_kernel(
    hidden, marks_row, marks_col, counts, gain, weights_hbm, out_w, down_t,
    out,
    w, own, w2, ones, parts, part_relay, arrived, share, pooled, latent, scaled, acc, kv, kv_all, query, mx, tot, mix, attn,
    far, relay_r, relay_l, to_right, to_left, arr_r, arr_l, lat_out, downs, down_relay, down_in, down_share, patch,
    lead, lead_in, trail, trail_in,
    w_sem, p_send, p_recv, s_send, s_recv, l_send, l_recv, f_send, f_recv, z_send, z_recv, x_send, x_recv,
    o_send, o_recv, d_send, d_recv, e_send, e_recv, lead_send, lead_recv, trail_send, trail_recv,
    own_sem, g_send, g_recv,
):
    ctx, tp, dp = position()
    h, x = ctx // 4, ctx % 4
    load = pltpu.make_async_copy(weights_hbm, w, w_sem)
    load.start()
    loads = [pltpu.make_async_copy(out_w, own.at[pl.ds(0, 512)], own_sem.at[0])]
    loads += [
        pltpu.make_async_copy(down_t.at[:, pl.ds(256 * i, 256)], own.at[pl.ds(512 + 64 * i, 64)], own_sem.at[1 + i])
        for i in range(4)
    ]
    for c in loads:
        c.start()
    gather = Gather(own, w2, g_send, g_recv)
    link = gather_links(ctx, tp, dp)
    tps = [(ctx, (tp + i) % 4, dp) for i in (1, 2, 3)]
    up_y, down_y = tps[0], tps[2]
    zs = [(((h + i) % 4) * 4 + x, tp, dp) for i in (1, 3)]
    right, left = (h * 4 + (x + 1) % 4, tp, dp), (h * 4 + (x + 3) % 4, tp, dp)
    next_first = ((ctx + 1) % 16, tp * 0, dp)
    before_all = [((ctx + 15) % 16, t, dp) for t in range(4)]
    barrier = pltpu.get_barrier_semaphore()

    def greet(devices):
        for device in devices:
            pl.semaphore_signal(barrier, inc=1, device_id=device, device_id_type=MESH)

    greet(tps + zs + [right, left, next_first] + [link[name] for name in ("E", "I", "D")])

    @pl.when(tp == 0)
    def _():
        greet(before_all)

    def dot(a, b):
        return jnp.dot(a, b, preferred_element_type=F32)

    def iota(shape, dim):
        return lax.broadcasted_iota(jnp.int32, shape, dim).astype(F32)

    ones[...] = jnp.ones_like(ones)
    r256, c256 = iota((256, 256), 0), iota((256, 256), 1)
    c4 = [counts[t].astype(F32) for t in range(4)]
    offset = jnp.zeros((8, 128), F32)
    for t in range(4):
        offset = offset + jnp.where(tp > t, c4[t], F32(0.0))
    group = c4[0] + c4[1] + c4[2] + c4[3]
    offset, group_one = offset[0:1, 0:1], group[0:1, 0:1]
    run_row = dot(marks_row[...], (r256 <= c256).astype(BF))
    run_col = dot((r256 >= c256).astype(BF), marks_col[...])[:, 0:1]
    slot_row = run_row[0:1] + offset - 1.0
    slot_col = run_col + offset - 1.0
    place = (r256 == slot_row).astype(BF)
    mass = dot(place, hidden[...])
    number = dot(place, ones[...])
    for t in range(4):
        parts[t, :, pl.ds(0, 1024)] = mass[64 * t : 64 * t + 64].astype(BF)
        parts[t, :, pl.ds(1024, 128)] = number[64 * t : 64 * t + 64].astype(BF)
    leading = (run_row == 0.0).astype(BF)
    lead[:, pl.ds(0, 1024)] = dot(leading, hidden[...])
    lead[:, pl.ds(1024, 128)] = dot(leading, ones[...])

    pl.semaphore_wait(barrier, 11 + 4 * (tp == 0).astype(jnp.int32))

    leads = [remote(lead.at[pl.ds(0, 8)], lead_in, lead_send.at[t], lead_recv, before_all[t]) for t in range(4)]

    @pl.when(tp == 0)
    def _():
        for c in leads:
            c.start()

    opposite, above, below = (tp + 2) % 4, (tp + 1) % 4, (tp + 3) % 4
    half_a, half_b = pl.ds(0, 32), pl.ds(32, 32)

    def scatter(src, relay, dst, send, recv):
        return [
            remote(src.at[opposite, half_a], relay.at[0], send.at[0], recv.at[0], up_y),
            remote(src.at[opposite, half_b], relay.at[1], send.at[1], recv.at[1], down_y),
            remote(src.at[above], dst.at[0], send.at[2], recv.at[2], up_y),
            remote(src.at[below], dst.at[1], send.at[3], recv.at[3], down_y),
        ]

    def pass_on(src, relay, copies):
        copies[0].wait_recv()
        src[above, half_a] = (src[above, half_a].astype(F32) + relay[0].astype(F32)).astype(BF)
        copies[2].start()
        copies[1].wait_recv()
        src[below, half_b] = (src[below, half_b].astype(F32) + relay[1].astype(F32)).astype(BF)
        copies[3].start()

    def gathered(src, dst, copies):
        copies[2].wait_recv()
        copies[3].wait_recv()
        return src[tp].astype(F32) + dst[0].astype(F32) + dst[1].astype(F32)

    def spread(src, dst, send, recv):
        lower, upper = dst.at[below, half_a], dst.at[above, half_b]
        return [
            remote(src, dst.at[tp], send.at[0], recv.at[0], up_y),
            remote(src, dst.at[tp], send.at[1], recv.at[1], down_y),
            remote(lower, lower, send.at[2], recv.at[2], up_y),
            remote(upper, upper, send.at[3], recv.at[3], down_y),
        ]

    def spread_rest(copies):
        for i in (0, 1):
            copies[i].wait_recv()
            copies[2 + i].start()
        for i in (2, 3):
            copies[i].wait_recv()

    first = scatter(parts, part_relay, arrived, p_send, p_recv)
    for c in first[:2]:
        c.start()
    for c in loads:
        c.wait()
    gather.until(0.0)
    w2[pl.ds(h, 1), pl.ds(x, 1)] = own[...][None, None]
    pass_on(parts, part_relay, first)
    gather.until(7.0)
    sums = gathered(parts, arrived, first)
    leads[0].wait_recv()
    my_row = iota((64, 1152), 0) + (64 * tp).astype(F32)
    sums = sums + jnp.where(my_row == group_one - 1.0, lead_in[0:1], F32(0.0))
    share[...] = (sums[:, :1024] / jnp.maximum(sums[:, 1024:1025], 1.0)).astype(BF)
    second = spread(share, pooled, s_send, s_recv)
    for c in second[:2]:
        c.start()
    pooled[pl.ds(tp, 1)] = share[...][None]
    load.wait()
    gather.until(14.0)
    spread_rest(second)

    def columns(t, i):
        return pl.ds(pl.multiple_of(1024 * t + 256 * i, 256), 256)

    def sent(i):
        block = latent.at[:, columns(tp, i)]
        return [
            remote(block, block, l_send.at[i], l_recv.at[i], up_y),
            remote(block, block, l_send.at[4 + i], l_recv.at[4 + i], down_y),
        ]

    def passed(i):
        block = latent.at[:, columns((tp + 3) % 4 if i < 2 else (tp + 1) % 4, i)]
        return remote(block, block, f_send.at[i], f_recv.at[i], up_y if i < 2 else down_y)

    all_pooled = pooled[...].reshape(256, 1024)
    for i in range(4):
        block = w[:, :, pl.ds(64 * i, 64), :].reshape(1024, 256)
        latent[:, columns(tp, i)] = dot(all_pooled, block).astype(BF)
        for c in sent(i):
            c.start()
    gather.until(18.0)

    def contract(t, i, fresh=False):
        values = latent[:, columns(t, i)].astype(F32)
        inputs = (values * gain[:, columns(t, i)]).astype(BF)
        power = jnp.sum(values * values, axis=-1, keepdims=True)
        scaled[...] = power if fresh else scaled[...] + power
        for b in range(3):
            term = dot(inputs, w[t, i, pl.ds(256 + 256 * b, 256), :])
            acc[b] = term if fresh else acc[b] + term

    for i in range(4):
        contract(tp, i, i == 0)
        gather.until(19.5 + 1.5 * i)
    for i in range(4):
        remote(latent.at[:, columns(tp, i)], latent.at[:, columns(tp, i)], l_send.at[i], l_recv.at[i], up_y).wait_recv()
        if i < 2:
            passed(i).start()
        remote(latent.at[:, columns(tp, i)], latent.at[:, columns(tp, i)], l_send.at[4 + i], l_recv.at[4 + i], down_y).wait_recv()
        if i >= 2:
            passed(i).start()
        contract((tp + 3) % 4, i)
        contract((tp + 1) % 4, i)
        gather.until(26.0 + 2.0 * i)
    for i in (0, 2, 1, 3):
        passed(i).wait_recv()
        contract((tp + 2) % 4, i)
    gather.until(35.0)
    scale = lax.rsqrt(scaled[...] * F32(1.0 / 4096.0) + EPS)
    kv[pl.ds(0, 256)] = (acc[2] * scale).astype(BF)
    kv[pl.ds(256, 16)] = jnp.broadcast_to(group_one, (16, 256)).astype(BF)

    low_rows, high_rows = pl.ds(0, 128), pl.ds(128, 144)
    z_low, z_high = kv_all.at[(h + 3) % 4, x, low_rows], kv_all.at[(h + 1) % 4, x, high_rows]
    z_copies = [remote(kv, kv_all.at[h, x], z_send.at[i], z_recv.at[i], zs[i]) for i in range(2)]
    z_copies.append(remote(z_low, z_low, z_send.at[2], z_recv.at[2], zs[0]))
    z_copies.append(remote(z_high, z_high, z_send.at[3], z_recv.at[3], zs[1]))
    for c in z_copies[:2]:
        c.start()

    def across(j, dz):
        z = (h + dz) % 4
        src = kv if dz == 0 else kv_all.at[z, x]
        lower, upper = pl.ds(0, 128), pl.ds(128, 144)
        a, b = (x + 3) % 4, (x + 1) % 4
        return [
            remote(src, kv_all.at[z, x], x_send.at[4 * j], x_recv.at[4 * j], right),
            remote(src, kv_all.at[z, x], x_send.at[4 * j + 1], x_recv.at[4 * j + 1], left),
            remote(kv_all.at[z, a, lower], kv_all.at[z, a, lower], x_send.at[4 * j + 2], x_recv.at[4 * j + 2], right),
            remote(kv_all.at[z, b, upper], kv_all.at[z, b, upper], x_send.at[4 * j + 3], x_recv.at[4 * j + 3], left),
        ]

    turns = (0, 3, 1, 2)
    sets = [across(j, dz) for j, dz in enumerate(turns)]
    sets[0][0].start()
    sets[0][1].start()
    kv_all[pl.ds(h, 1), pl.ds(x, 1)] = kv[...][None, None]
    for head in range(4):
        q = acc[head // 2][:, 128 * (head % 2) : 128 * (head % 2) + 128] * scale
        query[pl.ds(256 * head, 256)] = q.astype(BF)

    shrink = F32(1.0) / jnp.sqrt(F32(HEAD_SIZE))

    def attend(*chunks, fresh=False):
        places = [((h + dz) % 4, (x + dx) % 4) for dz, dx in chunks]
        seen = [z * 4 + xx <= ctx for z, xx in places]

        @pl.when(seen[0] if len(chunks) == 1 else seen[0] | seen[1])
        def _():
            joined, joined_v, biases = [], [], []
            for (z, xx), reached in zip(places, seen):
                joined.append(kv_all[z, xx, pl.ds(0, 256), pl.ds(0, 128)])
                joined_v.append(kv_all[z, xx, pl.ds(0, 256), pl.ds(128, 128)])
                limit = kv_all[z, xx, pl.ds(256, 16), :][0:1].astype(F32)
                limit = jnp.where(reached, limit, F32(0.0))
                biases.append(jnp.where(c256[0:1] < limit, F32(0.0), F32(-1e30)))
            keys, values, bias = joined[0], joined_v[0], biases[0]
            if len(chunks) == 2:
                keys, values = jnp.concatenate(joined, axis=0), jnp.concatenate(joined_v, axis=0)
                bias = jnp.concatenate(biases, axis=1)
            if fresh:
                causal = jnp.where(c256 <= r256, F32(0.0), F32(-1e30))
                bias = bias + jnp.concatenate([causal, causal], axis=0)

            def two_heads(i, carry):
                rows = pl.ds(pl.multiple_of(512 * i, 512), 512)
                s = nt(query[rows], keys) * shrink + bias
                peak = jnp.max(s, axis=-1, keepdims=True)
                if not fresh:
                    old = mx[rows]
                    peak = jnp.maximum(peak, old)
                e = jnp.exp(s - peak)
                total = jnp.sum(e, axis=-1, keepdims=True)
                mixed = dot(e.astype(BF), values)
                if not fresh:
                    fade = jnp.exp(old - peak)
                    total = total + tot[rows] * fade
                    mixed = mixed + mix[rows] * fade
                mx[rows] = peak
                tot[rows] = total
                mix[rows] = mixed
                return carry

            lax.fori_loop(0, 2, two_heads, 0)

    def along(j):
        sets[j][0].start()
        sets[j][1].start()

    def turn(j):
        for i in (0, 1):
            sets[j][i].wait_recv()
            sets[j][i + 2].start()

    attend((0, 0), fresh=True)
    gather.until(38.0)
    for i in (0, 1):
        z_copies[i].wait_recv()
        z_copies[i + 2].start()
        along(i + 1)
    turn(0)
    attend((3, 0), (1, 0))
    z_copies[2].wait_recv()
    z_copies[3].wait_recv()
    along(3)
    attend((0, 3), (0, 1))
    turn(1)
    gather.until(1000.0)
    turn(2)
    attend((3, 3), (3, 1))
    attend((2, 0))
    turn(3)
    attend((1, 3), (1, 1))
    attend((2, 3), (2, 1))
    for j in range(4):
        for i in (2, 3):
            sets[j][i].wait_recv()
        if j % 2:
            attend((turns[j - 1], 2), (turns[j], 2))
    for head in range(4):
        rows = pl.ds(256 * head, 256)
        attn[:, pl.ds(128 * head, 128)] = (mix[rows] / tot[rows]).astype(BF)

    def part(t, i):
        return dot(attn[...], w2[t, i, pl.ds(0, 512), :])

    def block(i):
        return pl.ds(256 * i, 256)

    low, high = pl.ds(0, 128), pl.ds(128, 128)
    for i in range(4):
        far[:, block(i)] = part(opposite, i).astype(BF)
    o_copies = [
        remote(far.at[low], relay_r, o_send.at[0], o_recv.at[0], up_y),
        remote(far.at[high], relay_l, o_send.at[1], o_recv.at[1], down_y),
        remote(to_right, arr_r, o_send.at[2], o_recv.at[2], up_y),
        remote(to_left, arr_l, o_send.at[3], o_recv.at[3], down_y),
    ]
    o_copies[0].start()
    o_copies[1].start()
    for i in range(4):
        acc_r = part(above, i)
        if i == 0:
            o_copies[0].wait_recv()
        to_right[low, block(i)] = (acc_r[:128] + relay_r[:, block(i)].astype(F32)).astype(BF)
        to_right[high, block(i)] = acc_r[128:].astype(BF)
    o_copies[2].start()
    for i in range(4):
        acc_l = part(below, i)
        if i == 0:
            o_copies[1].wait_recv()
        to_left[low, block(i)] = acc_l[:128].astype(BF)
        to_left[high, block(i)] = (acc_l[128:] + relay_l[:, block(i)].astype(F32)).astype(BF)
    o_copies[3].start()
    o_copies[2].wait_recv()
    o_copies[3].wait_recv()
    total_down = jnp.zeros((256, 1024), F32)
    for i in range(4):
        value = part(tp, i) + latent[:, columns(tp, i)].astype(F32)
        value = value + arr_r[:, block(i)].astype(F32) + arr_l[:, block(i)].astype(F32)
        lat_out[:, block(i)] = value.astype(BF)
    for i in range(4):
        down = w2[:, :, pl.ds(512 + 64 * i, 64), :].reshape(1024, 256)
        total_down = total_down + nt(lat_out[:, block(i)], down)
    for t in range(4):
        downs[t] = total_down[64 * t : 64 * t + 64].astype(BF)
    third = scatter(downs, down_relay, down_in, d_send, d_recv)
    for c in third[:2]:
        c.start()
    pass_on(downs, down_relay, third)
    sums = gathered(downs, down_in, third)
    down_share[...] = sums.astype(BF)
    final = (iota((16, 64), 1) + (64 * tp).astype(F32) == group_one - 1.0).astype(BF)
    trail[...] = dot(final, down_share[...]).astype(BF)
    fourth = spread(down_share, patch, e_send, e_recv)
    for c in fourth[:2]:
        c.start()
    trail_copies = [remote(trail, trail_in.at[t], trail_send, trail_recv.at[t], next_first) for t in range(4)]
    for t in range(4):

        @pl.when((tp == t) & (ctx < 15))
        def _():
            trail_copies[t].start()

    patch[pl.ds(tp, 1)] = down_share[...][None]
    spread_rest(fourth)
    patch_out = patch[...].reshape(256, 1024)
    result = hidden[...].astype(F32) + dot((c256 == slot_col).astype(BF), patch_out)
    out[...] = result.astype(BF)

    @pl.when((tp == 0) & (ctx > 0))
    def _():
        row = jnp.zeros((1, 1024), F32)
        for t in range(4):
            trail_copies[t].wait_recv()
            row = row + trail_in[t][0:1].astype(F32)
        out[...] = (out[...].astype(F32) + jnp.where(run_col == 0.0, row, F32(0.0))).astype(BF)

    @pl.when(ctx < 15)
    def _():
        trail_copies[0].wait_send()

    @pl.when(tp == 0)
    def _():
        for c in leads:
            c.wait_send()

    for c in first + second + third + fourth + z_copies + o_copies:
        c.wait_send()
    for i in range(4):
        for c in sent(i):
            c.wait_send()
        passed(i).wait_send()
    for group_of in sets:
        for c in group_of:
            c.wait_send()
    gather.drain()


def second_stage(hidden, marks_row, marks_col, counts, gain, weights, out_w, down_t):
    anywhere = pl.BlockSpec(memory_space=pl.ANY)
    vmem = pl.BlockSpec(memory_space=pltpu.VMEM)
    dma = pltpu.SemaphoreType.DMA

    n = len(PLANS[SECOND][1])

    def v(*shape, kind=BF):
        return pltpu.VMEM(shape, kind)

    return pl.pallas_call(
        second_kernel,
        out_shape=jax.ShapeDtypeStruct(hidden.shape, BF),
        in_specs=[vmem] * 5 + [anywhere] * 3,
        out_specs=vmem,
        scratch_shapes=[
            v(4, 4, FIRST, 256), v(SECOND, 256), v(4, 4, SECOND, 256), v(256, 128), v(4, 64, 1152), v(2, 32, 1152), v(2, 64, 1152), v(64, 1024), v(4, 64, 1024),
            v(256, 4096), v(256, 1, kind=F32), v(3, 256, 256, kind=F32), v(272, 256), v(4, 4, 272, 256),
            v(1024, 128), v(1024, 1, kind=F32), v(1024, 1, kind=F32), v(1024, 128, kind=F32), v(256, 512),
            v(256, 1024), v(128, 1024), v(128, 1024), v(256, 1024), v(256, 1024), v(256, 1024), v(256, 1024),
            v(256, 1024), v(4, 64, 1024), v(2, 32, 1024), v(2, 64, 1024), v(64, 1024), v(4, 64, 1024),
            v(16, 1152, kind=F32), v(8, 1152, kind=F32), v(16, 1024), v(4, 16, 1024),
            dma, dma((4,)), dma((4,)), dma((4,)), dma((4,)), dma((8,)), dma((8,)), dma((4,)), dma((4,)),
            dma((4,)), dma((4,)), dma((16,)), dma((16,)), dma((4,)), dma((4,)), dma((4,)), dma((4,)),
            dma((4,)), dma((4,)), dma((4,)), dma, dma, dma((4,)),
            dma((5,)), dma((n,)), dma((n,)),
        ],
        compiler_params=pltpu.CompilerParams(collective_id=1, has_side_effects=True, vmem_limit_bytes=62 * 2**20),
    )(hidden, marks_row, marks_col, counts, gain, weights, out_w, down_t)


def local(
    byte_embed, patch_start, enc_gain, enc_qkv, enc_out, up_proj, lat_gain, query_proj, key_proj,
    value_matrix, out_proj, down_proj,
):
    local_count = jnp.sum(patch_start)
    whole, hidden, counts = first_stage(
        up_proj, query_proj, key_proj, value_matrix, byte_embed,
        jnp.full((8, 128), local_count, jnp.int32), enc_gain[None, :], enc_qkv, enc_out,
    )
    marks = patch_start.astype(BF)
    marks_row = jnp.broadcast_to(marks[None, :], (16, 256))
    marks_col = jnp.broadcast_to(marks[:, None], (256, 128))
    return second_stage(hidden, marks_row, marks_col, counts, lat_gain[None, :], whole, out_proj, down_proj.T)


def solution(mesh):
    placed = (
        P(("dp", "ctx", "tp"), None), P(("dp", "ctx", "tp")), P(), P(), P(), P("ctx", "tp"), P(),
        P("ctx", "tp"), P("ctx", "tp"), P("ctx", "tp"), P("tp", "ctx"), P("tp", "ctx"),
    )
    return jax.shard_map(
        local, mesh=mesh, in_specs=placed, out_specs=P(("dp", "ctx", "tp"), None), check_vma=False
    )
```
